128 devices in a mesh: pod: 1, data: 64 (over z, y, x), seq: 2 (over core).
Axes of the slice: x: 4, y: 4, z: 4, core: 2. Of those that a mesh axis runs over, the one named last changes fastest.
Arguments:
- x_tokens: bfloat16 [64, 2048, 1024], P(('pod', 'data'), 'seq')
- w_query: bfloat16 [1024, 1024], replicated
- w_key: bfloat16 [1024, 1024], replicated
- w_value: bfloat16 [1024, 1024], replicated
- w_out: bfloat16 [16, 64, 1024], replicated
- dy_tokens: bfloat16 [64, 2048, 1024], P(('pod', 'data'), 'seq')
Outputs:
- output 1: bfloat16 [64, 2048, 1024], P(('pod', 'data'), 'seq')
- output 2: bfloat16 [64, 2048, 1024], P(('pod', 'data'), 'seq')
- output 3: float32 [4096, 1024], P(('pod', 'data'))
All inputs are finite; a program needn't handle non-finite values.
Results may differ from the reference program's by a relative error of at most 0.00966561.
Values are sent between devices in bfloat16 or wider.
A program may use at most 1 GiB of HBM per device.

```python
import math
import jax
import jax.numpy as jnp
from jax import lax

MODEL_DIM = 1024
NUM_HEADS = 16
HEAD_DIM = 64
NUM_SEQS = 64
SEQ_LEN = 2048

REF_BLOCK = math.gcd(SEQ_LEN, 256)
NUM_BLOCKS = SEQ_LEN // REF_BLOCK
ATTN_SCALE = (HEAD_DIM * SEQ_LEN) ** -0.5
FLAT_ROWS = NUM_SEQS * REF_BLOCK


def setup_inputs(seed: int = 0, part: int = 0) -> dict:
    part_key = jax.random.fold_in(jax.random.key(seed), part)
    key_x, key_dy = jax.random.split(part_key, 2)
    weight_keys = jax.random.split(jax.random.key(seed + 1), 4)
    shape_act = (NUM_SEQS, SEQ_LEN, MODEL_DIM)
    shape_w = (MODEL_DIM, MODEL_DIM)
    w_scale = MODEL_DIM ** -0.5
    x_tokens = jax.random.normal(key_x, shape_act, jnp.float32)
    dy_tokens = jax.random.normal(key_dy, shape_act, jnp.float32)
    w_query = jax.random.normal(weight_keys[0], shape_w, jnp.float32) * w_scale
    w_key = jax.random.normal(weight_keys[1], shape_w, jnp.float32) * w_scale
    w_value = jax.random.normal(weight_keys[2], shape_w, jnp.float32) * w_scale
    w_out = jax.random.normal(weight_keys[3], shape_w, jnp.float32) * w_scale
    return {
        "x_tokens": x_tokens.astype(jnp.bfloat16),
        "w_query": w_query.astype(jnp.bfloat16),
        "w_key": w_key.astype(jnp.bfloat16),
        "w_value": w_value.astype(jnp.bfloat16),
        "w_out": w_out.reshape(NUM_HEADS, HEAD_DIM, MODEL_DIM).astype(jnp.bfloat16),
        "dy_tokens": dy_tokens.astype(jnp.bfloat16),
    }


def silu_grad(pre_act):
    sigmoid_val = jax.nn.sigmoid(pre_act)
    return sigmoid_val * (1.0 + pre_act * (1.0 - sigmoid_val))


def to_heads(flat_val):
    return flat_val.reshape(NUM_SEQS, REF_BLOCK, NUM_HEADS, HEAD_DIM).astype(jnp.float32)


def features(x_blk, w_query, w_key, w_value):
    x_flat = x_blk.reshape(FLAT_ROWS, MODEL_DIM)
    q_pre = jnp.dot(x_flat, w_query, preferred_element_type=jnp.float32)
    k_pre = jnp.dot(x_flat, w_key, preferred_element_type=jnp.float32)
    v_pre = jnp.dot(x_flat, w_value, preferred_element_type=jnp.float32)
    q_feat = to_heads(jax.nn.silu(q_pre).astype(jnp.bfloat16))
    k_feat = to_heads(jax.nn.silu(k_pre).astype(jnp.bfloat16))
    v_feat = to_heads(v_pre.astype(jnp.bfloat16))
    return x_flat, q_pre, k_pre, q_feat, k_feat, v_feat


def grad_heads(dy_blk, wo_flat):
    dy_flat = dy_blk.reshape(FLAT_ROWS, MODEL_DIM)
    d_attn = jnp.dot(dy_flat, wo_flat.T, preferred_element_type=jnp.float32).astype(jnp.bfloat16)
    return dy_flat, to_heads(d_attn)


def reference(x_tokens, w_query, w_key, w_value, w_out, dy_tokens):
    wo_flat = w_out.reshape(MODEL_DIM, MODEL_DIM)
    causal = jnp.tril(jnp.ones((REF_BLOCK, REF_BLOCK), jnp.float32))
    blocked = (NUM_SEQS, NUM_BLOCKS, REF_BLOCK, MODEL_DIM)
    out_shape = (NUM_SEQS, REF_BLOCK, MODEL_DIM)
    x_blocks = x_tokens.reshape(blocked).transpose(1, 0, 2, 3)
    dy_blocks = dy_tokens.reshape(blocked).transpose(1, 0, 2, 3)

    def forward_step(carry, blocks):
        kv_state, dwo_sum = carry
        x_blk, dy_blk = blocks
        x_flat, q_pre, k_pre, q_feat, k_feat, v_feat = features(x_blk, w_query, w_key, w_value)
        scores = jnp.einsum("bthk,bshk->bhts", q_feat, k_feat) * causal
        intra_part = jnp.einsum("bhts,bshv->bthv", scores, v_feat)
        inter_part = jnp.einsum("bthk,bhkv->bthv", q_feat, kv_state)
        attn_out = (ATTN_SCALE * (intra_part + inter_part)).astype(jnp.bfloat16).reshape(FLAT_ROWS, MODEL_DIM)
        y_blk = jnp.dot(attn_out, wo_flat, preferred_element_type=jnp.float32).astype(jnp.bfloat16)
        dy_flat, d_attn = grad_heads(dy_blk, wo_flat)
        dv_scores = jnp.einsum("bthv,bshv->bhts", d_attn, v_feat) * causal
        dq_val = jnp.einsum("bhts,bshk->bthk", dv_scores, k_feat) + jnp.einsum("bthv,bhkv->bthk", d_attn, kv_state)
        grad_q = (ATTN_SCALE * dq_val.reshape(FLAT_ROWS, MODEL_DIM) * silu_grad(q_pre)).astype(jnp.bfloat16)
        kv_state = kv_state + jnp.einsum("bthk,bthv->bhkv", k_feat, v_feat)
        dwo_sum = dwo_sum + jnp.dot(attn_out.T, dy_flat, preferred_element_type=jnp.float32)
        return (kv_state, dwo_sum), (y_blk.reshape(out_shape), grad_q.reshape(out_shape))

    def reverse_step(carry, blocks):
        rev_state, dwq_sum, dwk_sum, dwv_sum = carry
        x_blk, dy_blk, gq_blk = blocks
        x_flat, q_pre, k_pre, q_feat, k_feat, v_feat = features(x_blk, w_query, w_key, w_value)
        dy_flat, d_attn = grad_heads(dy_blk, wo_flat)
        scores = jnp.einsum("bthk,bshk->bhts", q_feat, k_feat) * causal
        dv_scores = jnp.einsum("bthv,bshv->bhts", d_attn, v_feat) * causal
        dk_val = jnp.einsum("bhts,bthk->bshk", dv_scores, q_feat) + jnp.einsum("bshv,bhkv->bshk", v_feat, rev_state)
        dv_val = jnp.einsum("bhts,bthv->bshv", scores, d_attn) + jnp.einsum("bshk,bhkv->bshv", k_feat, rev_state)
        grad_q = gq_blk.reshape(FLAT_ROWS, MODEL_DIM)
        grad_k = (ATTN_SCALE * dk_val.reshape(FLAT_ROWS, MODEL_DIM) * silu_grad(k_pre)).astype(jnp.bfloat16)
        grad_v = (ATTN_SCALE * dv_val.reshape(FLAT_ROWS, MODEL_DIM)).astype(jnp.bfloat16)
        rev_state = rev_state + jnp.einsum("bthk,bthv->bhkv", q_feat, d_attn)
        dx_val = (jnp.dot(grad_q, w_query.T, preferred_element_type=jnp.float32)
                  + jnp.dot(grad_k, w_key.T, preferred_element_type=jnp.float32)
                  + jnp.dot(grad_v, w_value.T, preferred_element_type=jnp.float32))
        dwq_sum = dwq_sum + jnp.dot(x_flat.T, grad_q, preferred_element_type=jnp.float32)
        dwk_sum = dwk_sum + jnp.dot(x_flat.T, grad_k, preferred_element_type=jnp.float32)
        dwv_sum = dwv_sum + jnp.dot(x_flat.T, grad_v, preferred_element_type=jnp.float32)
        return (rev_state, dwq_sum, dwk_sum, dwv_sum), dx_val.astype(jnp.bfloat16).reshape(out_shape)

    zero_state = jnp.zeros((NUM_SEQS, NUM_HEADS, HEAD_DIM, HEAD_DIM), jnp.float32)
    zero_mat = jnp.zeros((MODEL_DIM, MODEL_DIM), jnp.float32)
    fwd_carry, fwd_outs = lax.scan(forward_step, (zero_state, zero_mat), (x_blocks, dy_blocks))
    y_blocks, gq_blocks = fwd_outs
    rev_carry, dx_blocks = lax.scan(reverse_step, (zero_state, zero_mat, zero_mat, zero_mat), (x_blocks, dy_blocks, gq_blocks), reverse=True)
    y_tokens = y_blocks.transpose(1, 0, 2, 3).reshape(NUM_SEQS, SEQ_LEN, MODEL_DIM)
    dx_tokens = dx_blocks.transpose(1, 0, 2, 3).reshape(NUM_SEQS, SEQ_LEN, MODEL_DIM)
    dw_shards = jnp.concatenate([rev_carry[1], rev_carry[2], rev_carry[3], fwd_carry[1]], axis=0)
    return y_tokens, dx_tokens, dw_shards
```

```python
import jax
import jax.numpy as jnp
from jax import lax
from jax.experimental import pallas as pl
from jax.experimental.pallas import tpu as pltpu
from jax.sharding import PartitionSpec as P

MESH = pl.DeviceIdType.MESH
F32 = jnp.float32
BF16 = jnp.bfloat16

TOK = 1024
SEQ = 2 * TOK
DIM = 1024
HALF = DIM // 2
GRP = 256
CHUNK = 256
NCH = SEQ // CHUNK
BLK = 512
ROWS = 64

ORDER = (("z", "y", "x"), ("y", "x", "z"), ("x", "z", "y"))
PART_ROWS = ((0, 16), (16, 24), (40, 24))
AXES = ("z", "y", "x")


def dot(a, b):
    return lax.dot_general(a, b, (((1,), (0,)), ((), ())), preferred_element_type=F32)


def dot_t(a, b):
    return lax.dot_general(a, b, (((1,), (1,)), ((), ())), preferred_element_type=F32)


def t_dot(a, b):
    return lax.dot_general(a, b, (((0,), (0,)), ((), ())), preferred_element_type=F32)


class Ids:
    def __init__(self):
        self.n = 0

    def take(self):
        self.n += 1
        return self.n - 1


NUM_SEMS = 128
NUM_LOCAL = 16


def kernel(scale, x_hbm, dy_hbm, wq_hbm, wk_hbm, wv_hbm, wo_hbm,
           y_hbm, dx_hbm, dw_ref,
           xf, xt, dyf, wq, wk, wv, wo, sga, sgb, qg, kg, vg, dog,
           pre, pre_t, suf, suf_t, state, oo, o_in, gq, gk, gv, g_in, acc, fin,
           r00, l00, m00, r01, l01, m01, r02, l02, m02,
           r10, l10, m10, r11, l11, m11, r12, l12, m12,
           r20, l20, m20, r21, l21, m21, r22, l22, m22,
           send_sem, recv_sem, local_sem):
    core = lax.axis_index("seq")
    data = lax.axis_index("data")
    me = {"z": data // 16, "y": (data // 4) % 4, "x": data % 4}
    other = 1 - core
    hop_bufs = {(0, 0): (r00, l00, m00), (0, 1): (r01, l01, m01), (0, 2): (r02, l02, m02),
                (1, 0): (r10, l10, m10), (1, 1): (r11, l11, m11), (1, 2): (r12, l12, m12),
                (2, 0): (r20, l20, m20), (2, 1): (r21, l21, m21), (2, 2): (r22, l22, m22)}
    ids = Ids()
    sent = []

    def device(axis, delta):
        c = dict(me)
        c[axis] = (c[axis] + delta + 4) % 4
        return {"data": (c["z"] * 4 + c["y"]) * 4 + c["x"], "seq": core}

    partner = {"data": data, "seq": other}

    def remote(src, dst, dev):
        k = ids.take()
        return pltpu.make_async_remote_copy(src_ref=src, dst_ref=dst, send_sem=send_sem.at[k],
                                            recv_sem=recv_sem.at[k], device_id=dev, device_id_type=MESH)

    def start(copy):
        copy.start()
        sent.append(copy)

    def acc_slice(part, phase, g, h, j, m=None):
        r0, nr = PART_ROWS[part]
        where = {}
        for p, axis in enumerate(ORDER[part]):
            where[axis] = me[axis] if p < phase else j if p == phase else slice(None)
        if m is not None:
            where["z"] = m
        return acc.at[(g, h, where["z"], where["y"], where["x"], pl.ds(r0, nr), slice(None))]

    def buf_slice(buf, part, phase, g, h, m=None):
        rest = [a for a in AXES if a in ORDER[part][phase + 1:]]
        idx = [h, g] + [m if (a == "z" and m is not None) else slice(None) for a in rest]
        return buf.at[tuple(idx)]

    def hop_copies(part, phase, g, m=None):
        axis = ORDER[part][phase]
        i = me[axis]
        from_opp, from_left, from_right = hop_bufs[part, phase]
        c_opp, c_r, c_l = (i + 2) % 4, (i + 1) % 4, (i + 3) % 4
        right, left = device(axis, 1), device(axis, -1)
        mk = lambda h, j, buf, dev: remote(acc_slice(part, phase, g, h, j, m), buf_slice(buf, part, phase, g, h, m), dev)
        return {
            "1A": mk(0, c_opp, from_opp, right), "1B": mk(1, c_opp, from_opp, left),
            "RB": mk(1, c_r, from_left, right), "LA": mk(0, c_l, from_right, left),
            "RA": mk(0, c_r, from_left, right), "LB": mk(1, c_l, from_right, left),
            "key": (part, phase, g, m),
        }

    def hop_start(c):
        for k in ("1A", "1B", "RB", "LA"):
            start(c[k])

    def add_into(part, phase, g, m, h, j, bufs):
        rest = [a for a in AXES if a in ORDER[part][phase + 1:]]
        r0, nr = PART_ROWS[part]
        g_list = [g] if isinstance(g, int) else list(range(2))
        m_list = ([m] if isinstance(m, int) else list(range(4)) if m is None else list(range(3)))
        for gi in g_list:
            grid = [()]
            for a in rest:
                vals = m_list if a == "z" else range(4)
                grid = [t + (v,) for t in grid for v in vals]
            for t in grid:
                where = {}
                for p, axis in enumerate(ORDER[part]):
                    where[axis] = me[axis] if p < phase else j if p == phase else t[rest.index(axis)]
                at = (gi, h, where["z"], where["y"], where["x"], pl.ds(r0, nr), slice(None))
                total = acc[at]
                for b in bufs:
                    total = total + b[(h, gi) + t + (slice(None), slice(None))]
                acc[at] = total

    def hop_relay(c):
        part, phase, g, m = c["key"]
        i = me[ORDER[part][phase]]
        from_opp, _, _ = hop_bufs[part, phase]
        c["1A"].wait_recv()
        add_into(part, phase, g, m, 0, (i + 1) % 4, [from_opp])
        start(c["RA"])
        c["1B"].wait_recv()
        add_into(part, phase, g, m, 1, (i + 3) % 4, [from_opp])
        start(c["LB"])

    def hop_finish(c):
        part, phase, g, m = c["key"]
        i = me[ORDER[part][phase]]
        _, from_left, from_right = hop_bufs[part, phase]
        for k in ("RB", "LA", "RA", "LB"):
            c[k].wait_recv()
        for h in range(2):
            add_into(part, phase, g, m, h, i, [from_left, from_right])

    both = slice(None)
    low = pl.ds(0, 3)
    E = [{p: hop_copies(p, 0, g, low) for p in (1, 2)} for g in range(2)]
    L = {p: hop_copies(p, 0, both, 3) for p in (1, 2)}
    Z = hop_copies(0, 0, both)
    P2 = {p: hop_copies(p, 1, both) for p in range(3)}
    P3 = {p: hop_copies(p, 2, both) for p in range(3)}

    own0 = pl.multiple_of(core * TOK, TOK)
    oth0 = pl.multiple_of(other * TOK, TOK)
    loads = {}
    for k, (name, src, dst) in enumerate([
            ("x", x_hbm, xf.at[pl.ds(own0, TOK)]), ("wq", wq_hbm, wq), ("wk", wk_hbm, wk), ("wv", wv_hbm, wv),
            ("wo", wo_hbm, wo), ("dy", dy_hbm, dyf.at[pl.ds(own0, TOK)])]):
        loads[name] = pltpu.make_async_copy(src, dst, local_sem.at[k])
        loads[name].start()
    barrier = pltpu.get_barrier_semaphore()
    for dev in [partner] + [device(a, s) for a in AXES for s in (1, -1)]:
        pl.semaphore_signal(barrier, inc=1, device_id=dev, device_id_type=MESH)
    pl.semaphore_wait(barrier, 7)
    x_send = remote(x_hbm, xf.at[pl.ds(own0, TOK)], partner)
    dy_send = remote(dy_hbm, dyf.at[pl.ds(own0, TOK)], partner)
    start(x_send)
    start(dy_send)

    lanes = lax.broadcasted_iota(jnp.int32, (1, 128), 1)
    first = (lanes < 64).astype(F32).astype(BF16)
    second = (lanes >= 64).astype(F32).astype(BF16)
    causal = (lax.broadcasted_iota(jnp.int32, (CHUNK, CHUNK), 0)
              >= lax.broadcasted_iota(jnp.int32, (CHUNK, CHUNK), 1))
    block_diag = ((lax.broadcasted_iota(jnp.int32, (128, 128), 0) < 64)
                  == (lax.broadcasted_iota(jnp.int32, (128, 128), 1) < 64))

    def project(g, base0):
        off = pl.multiple_of(core * HALF + g * GRP, GRP)

        def body(i, _):
            base = pl.multiple_of(base0 + i * BLK, BLK)
            rows = pl.ds(base, BLK)
            xa = xf[rows, :]
            if g == 0:
                xt[:, rows] = xa.T
            for w, sg, out in ((wq, sga, qg), (wk, sgb, kg)):
                a = dot(xa, w[:, pl.ds(off, GRP)])
                s = jax.nn.sigmoid(a)
                out[rows, :] = (a * s).astype(BF16)
                sg[rows, :] = s * (1.0 + a * (1.0 - s))
            vg[rows, :] = dot(xa, wv[:, pl.ds(off, GRP)]).astype(BF16)
            dog[rows, :] = dot_t(dyf[rows, :], wo[pl.ds(off, GRP), :]).astype(BF16)
            return 0

        lax.fori_loop(0, TOK // BLK, body, 0)

    def scan_states():
        for a_ref, b_ref, out, out_t, order in ((kg, vg, pre, pre_t, 1), (qg, dog, suf, suf_t, -1)):
            for j in range(2):
                state[j] = jnp.zeros((128, 128), F32)

            def body(n, _):
                i = n if order == 1 else NCH - 1 - n
                rows = pl.ds(pl.multiple_of(i * CHUNK, CHUNK), CHUNK)
                for j in range(2):
                    cols = pl.ds(j * 128, 128)
                    st = state[j]
                    stb = st.astype(BF16)
                    out[i, j] = stb
                    out_t[i, j] = stb.T
                    kv = t_dot(a_ref[rows, cols], b_ref[rows, cols])
                    state[j] = st + jnp.where(block_diag, kv, 0.0)
                return 0

            lax.fori_loop(0, NCH, body, 0)

    def attend(g):
        def body(i, _):
            rows = pl.ds(pl.multiple_of(i * CHUNK, CHUNK), CHUNK)
            for j in range(2):
                cols = pl.ds(j * 128, 128)
                ocols = pl.ds(g * GRP + j * 128, 128)
                q, k, v, do = qg[rows, cols], kg[rows, cols], vg[rows, cols], dog[rows, cols]
                qa, qb, ka, kb = q * first, q * second, k * first, k * second
                va, vb, da, db = v * first, v * second, do * first, do * second
                p_a = jnp.where(causal, dot_t(qa, k), 0.0).astype(BF16)
                p_b = jnp.where(causal, dot_t(qb, k), 0.0).astype(BF16)
                d_a = jnp.where(causal, dot_t(da, v), 0.0).astype(BF16)
                d_b = jnp.where(causal, dot_t(db, v), 0.0).astype(BF16)
                o = dot(p_a, va) + dot(p_b, vb) + dot(q, pre[i, j])
                oo[rows, ocols] = (scale * o).astype(BF16)
                dq = dot(d_a, ka) + dot(d_b, kb) + dot(do, pre_t[i, j])
                gq[rows, ocols] = (scale * dq * sga[rows, cols]).astype(BF16)
                dk = t_dot(d_a, qa) + t_dot(d_b, qb) + dot(v, suf_t[i, j])
                gk[rows, ocols] = (scale * dk * sgb[rows, cols]).astype(BF16)
                dv = t_dot(p_a, da) + t_dot(p_b, db) + dot(k, suf[i, j])
                gv[rows, ocols] = (scale * dv).astype(BF16)
            return 0

        lax.fori_loop(0, NCH, body, 0)

    def weight_grads(g):
        cols = pl.ds(g * GRP, GRP)
        for m, gr in enumerate((gq, gk, gv)):
            def body(n, _):
                lhs = xt[pl.ds(pl.multiple_of(n * 512, 512), 512), :]
                t = dot(lhs, gr[:, cols])
                for h in range(2):
                    for yy in range(2):
                        for xx in range(4):
                            r = yy * 256 + xx * 64
                            acc[g, h, m, n * 2 + yy, xx] = t[r:r + 64, h * 128:h * 128 + 128]
                return 0

            lax.fori_loop(0, 2, body, 0)

    o_sends, g_sends = [], []
    for g in range(2):
        cols = pl.ds(g * GRP, GRP)
        if g == 0:
            for name in ("x", "wq", "wk", "wv", "wo", "dy"):
                loads[name].wait()
        project(g, core * TOK)
        if g == 0:
            x_send.wait_recv()
            dy_send.wait_recv()
        project(g, other * TOK)
        scan_states()
        if g == 1:
            for p in (1, 2):
                hop_relay(E[0][p])
        attend(g)
        o_sends.append(remote(oo.at[:, cols], o_in.at[:, cols], partner))
        start(o_sends[-1])
        for m, gr in enumerate((gq, gk, gv)):
            g_sends.append(remote(gr.at[pl.ds(oth0, TOK), cols], g_in.at[m, :, cols], partner))
            start(g_sends[-1])
        if g == 1:
            for p in (1, 2):
                hop_finish(E[0][p])
        weight_grads(g)
        for p in (1, 2):
            hop_start(E[g][p])

    for s in o_sends:
        s.wait_recv()

    def dwo(src, first_row_block):
        def body(n, _):
            lhs = src[:, pl.ds(pl.multiple_of(n * 256, 256), 256)]
            t = t_dot(lhs, dyf[:, pl.ds(pl.multiple_of(core * HALF, HALF), HALF)])
            for g in range(2):
                for h in range(2):
                    for xx in range(4):
                        acc[g, h, 3, first_row_block + n, xx] = t[xx * 64:xx * 64 + 64, g * 256 + h * 128:g * 256 + h * 128 + 128]
            return 0

        lax.fori_loop(0, 2, body, 0)

    dwo(oo, core * 2)
    dwo(o_in, other * 2)
    hop_start(Z)
    for p in (1, 2):
        hop_start(L[p])

    own_c = pl.ds(pl.multiple_of(core * HALF, HALF), HALF)
    oth_c = pl.ds(pl.multiple_of(other * HALF, HALF), HALF)

    def y_body(n, _):
        rows = pl.ds(pl.multiple_of(own0 + n * 512, 512), 512)
        t = dot(oo[rows, :], wo[own_c, :]) + dot(o_in[rows, :], wo[oth_c, :])
        xf[pl.ds(pl.multiple_of(n * 512, 512), 512), :] = t.astype(BF16)
        return 0

    def dx_body(n, _):
        rows = pl.ds(pl.multiple_of(own0 + n * 512, 512), 512)
        r = pl.ds(pl.multiple_of(n * 512, 512), 512)
        t = None
        for m, (gr, w) in enumerate(((gq, wq), (gk, wk), (gv, wv))):
            u = dot_t(gr[rows, :], w[:, own_c]) + dot_t(g_in[m, r, :], w[:, oth_c])
            t = u if t is None else t + u
        xf[pl.ds(pl.multiple_of(TOK + n * 512, 512), 512), :] = t.astype(BF16)
        return 0

    lax.fori_loop(0, 2, y_body, 0)
    y_out = pltpu.make_async_copy(xf.at[pl.ds(0, TOK)], y_hbm, local_sem.at[6])
    y_out.start()
    for p in (1, 2):
        hop_relay(E[1][p])
    hop_relay(Z)
    for p in (1, 2):
        hop_relay(L[p])
    for s in g_sends:
        s.wait_recv()
    lax.fori_loop(0, 2, dx_body, 0)
    dx_out = pltpu.make_async_copy(xf.at[pl.ds(TOK, TOK)], dx_hbm, local_sem.at[7])
    dx_out.start()

    for p in (1, 2):
        hop_finish(E[1][p])
        hop_finish(L[p])
        hop_start(P2[p])
    hop_finish(Z)
    hop_start(P2[0])
    for p in (1, 2, 0):
        hop_relay(P2[p])
    for p in (1, 2, 0):
        hop_finish(P2[p])
        hop_start(P3[p])
    for p in (1, 2, 0):
        hop_relay(P3[p])
    for p in (1, 2, 0):
        hop_finish(P3[p])

    final = acc.at[:, :, me["z"], me["y"], me["x"]]
    last = remote(final, fin, partner)
    start(last)
    for g in range(2):
        for h in range(2):
            at = pl.ds(pl.multiple_of(core * HALF + g * 256 + h * 128, 128), 128)
            dw_ref[:, at] = acc[g, h, me["z"], me["y"], me["x"]]
    last.wait_recv()
    for g in range(2):
        for h in range(2):
            at = pl.ds(pl.multiple_of(other * HALF + g * 256 + h * 128, 128), 128)
            dw_ref[:, at] = fin[g, h]
    for s in sent:
        s.wait_send()
    y_out.wait()
    dx_out.wait()
    assert ids.n <= NUM_SEMS, ids.n


def hop_shapes(part, phase):
    rest = len(ORDER[part]) - phase - 1
    shape = (2, 2) + (4,) * rest + (PART_ROWS[part][1], 128)
    return [pltpu.VMEM(shape, F32)] * 3


def solution(mesh):
    act = P(("pod", "data"), "seq", None)
    scale = float((64 * SEQ) ** -0.5)

    def local(x, wq, wk, wv, wo, dy):
        vm = pltpu.VMEM
        any_ = pl.BlockSpec(memory_space=pl.ANY)
        scratch = [
            vm((SEQ, DIM), BF16), vm((DIM, SEQ), BF16), vm((SEQ, DIM), BF16),
            *[vm((DIM, DIM), BF16)] * 4,
            *[vm((SEQ, GRP), F32)] * 2, *[vm((SEQ, GRP), BF16)] * 4,
            *[vm((NCH, 2, 128, 128), BF16)] * 4, vm((2, 128, 128), F32),
            vm((SEQ, HALF), BF16), vm((SEQ, HALF), BF16), *[vm((SEQ, HALF), BF16)] * 3, vm((3, TOK, HALF), BF16),
            vm((2, 2, 4, 4, 4, ROWS, 128), F32), vm((2, 2, ROWS, 128), F32),
        ]
        for part in range(3):
            for phase in range(3):
                scratch += hop_shapes(part, phase)
        scratch += [pltpu.SemaphoreType.DMA((NUM_SEMS,)), pltpu.SemaphoreType.DMA((NUM_SEMS,)),
                    pltpu.SemaphoreType.DMA((NUM_LOCAL,))]
        y, dx, dw = pl.pallas_call(
            lambda *refs: kernel(scale, *refs),
            out_shape=(jax.ShapeDtypeStruct((TOK, DIM), BF16), jax.ShapeDtypeStruct((TOK, DIM), BF16),
                       jax.ShapeDtypeStruct((ROWS, DIM), F32)),
            in_specs=[any_] * 6,
            out_specs=(any_, any_, pl.BlockSpec(memory_space=pltpu.VMEM)),
            scratch_shapes=scratch,
            name="layer",
            compiler_params=pltpu.CompilerParams(collective_id=0, has_side_effects=True, vmem_limit_bytes=67043328),
        )(x[0], dy[0], wq, wk, wv, wo.reshape(DIM, DIM))
        return y[None], dx[None], dw

    return jax.shard_map(local, mesh=mesh,
                         in_specs=(act, P(None, None), P(None, None), P(None, None), P(None, None, None), act),
                         out_specs=(act, act, P(("pod", "data"), None)), check_vma=False)
```

```python
import jax
import jax.numpy as jnp
from jax import lax
from jax.experimental import pallas as pl
from jax.experimental.pallas import tpu as pltpu
from jax.sharding import PartitionSpec as P

MESH = pl.DeviceIdType.MESH
F32 = jnp.float32
BF16 = jnp.bfloat16

TOK = 1024
SEQ = 2 * TOK
DIM = 1024
HALF = DIM // 2
GRP = 256
CHUNK = 256
NCH = SEQ // CHUNK
BLK = 512
ROWS = 64

ORDER = (("z", "y", "x"), ("y", "x", "z"), ("x", "z", "y"))
PART_ROWS = ((0, 16), (16, 24), (40, 24))
AXES = ("z", "y", "x")


def dot(a, b):
    return lax.dot_general(a, b, (((1,), (0,)), ((), ())), preferred_element_type=F32)


def dot_t(a, b):
    return lax.dot_general(a, b, (((1,), (1,)), ((), ())), preferred_element_type=F32)


def t_dot(a, b):
    return lax.dot_general(a, b, (((0,), (0,)), ((), ())), preferred_element_type=F32)


NUM_SEMS = 240
NUM_LOCAL = 12
KINDS = {"1A": (0, 2, 0, 1), "1B": (1, 2, 0, -1), "RB": (1, 1, 1, 1), "LA": (0, 3, 2, -1),
         "RA": (0, 1, 1, 1), "LB": (1, 3, 2, -1),
         "O": (slice(None), 2, 0, 2), "R": (slice(None), 1, 1, 1), "L": (slice(None), 3, 2, -1)}
RAW = ("1A", "1B", "RB", "LA")
RING = ("RB", "LA", "RA", "LB")
LAST = ("O", "R", "L")
GENS = {"E0": (0, 0, 3, None), "L0": (None, 3, 1, 0), "E1": (1, 0, 3, None), "L1": (None, 3, 1, 1)}


def when(cond, fn):
    if cond is None:
        fn()
    else:
        pl.when(cond)(fn)


def both(a, b):
    return b if a is None else a if b is None else jnp.logical_and(a, b)


def kernel(scale, x_hbm, dy_hbm, wq_hbm, wk_hbm, wv_hbm, wo_hbm,
           y_ref, dx_ref, dw_ref,
           xf, xt, dyf, wq, wk, wv, wo, sga, sgb, qg, kg, vg,
           kv_raw, qd_raw, oo, o_in, gq, gk, gv, g_in, acc, fin,
           r00, l00, m00, r01, l01, m01, r02, l02, m02,
           r10, l10, m10, r11, l11, m11, r12, l12, m12,
           r20, l20, m20, r21, l21, m21, r22, l22, m22,
           send_sem, recv_sem, local_sem):
    core = lax.axis_index("seq")
    data = lax.axis_index("data")
    me = {"z": lax.div(data, 16), "y": lax.rem(lax.div(data, 4), 4), "x": lax.rem(data, 4)}
    at = {a: [me[a]] + [lax.rem(me[a] + k, 4) for k in (1, 2, 3)] for a in AXES}
    yat = [lax.rem(v, 2) * 2 + lax.div(v, 2) for v in at["y"]]
    stride = {"z": 16, "y": 4, "x": 1}
    away = {a: [data + (at[a][k] - me[a]) * stride[a] for k in range(4)] for a in AXES}
    is_last = [v == 3 for v in at["z"]]
    not_last = [v != 3 for v in at["z"]]
    parity = [[lax.rem(v, 2) == par for v in at["y"]] for par in (0, 1)]
    conds = {}
    other = 1 - core
    hop_bufs = {(0, 0): (r00, l00, m00), (0, 1): (r01, l01, m01), (0, 2): (r02, l02, m02),
                (1, 0): (r10, l10, m10), (1, 1): (r11, l11, m11), (1, 2): (r12, l12, m12),
                (2, 0): (r20, l20, m20), (2, 1): (r21, l21, m21), (2, 2): (r22, l22, m22)}
    sem_ids = {}
    sent = []

    def device(axis, delta):
        return {"data": away[axis][delta % 4], "seq": core}

    partner = {"data": data, "seq": other}

    def remote(name, src, dst, dev):
        k = sem_ids.setdefault(name, len(sem_ids))
        assert k < NUM_SEMS
        return pltpu.make_async_remote_copy(src_ref=src, dst_ref=dst, send_sem=send_sem.at[k],
                                            recv_sem=recv_sem.at[k], device_id=dev, device_id_type=MESH)

    def start(copy):
        copy.start()
        sent.append((copy, None))

    def gen_test(gen, axis, k):
        _, m_lo, _, par = GENS[gen]
        if axis == "z":
            return ("z", m_lo != 0, k)
        if axis == "y" and par is not None:
            return ("y", par, k)
        return None

    def active(gen, part, phase, step):
        tests = [gen_test(gen, axis, 0 if p < phase else step) for p, axis in enumerate(ORDER[part][:phase + 1])]
        key = tuple(sorted(t for t in tests if t is not None))
        if key not in conds:
            cond = None
            for axis, kind, k in key:
                cond = both(cond, (is_last if kind else not_last)[k] if axis == "z" else parity[kind][k])
            conds[key] = cond
        return conds[key]

    def place(part, phase, step):
        where = {}
        for p, a in enumerate(ORDER[part][:phase + 1]):
            k = 0 if p < phase else step
            where[a] = yat[k] if a == "y" else at[a][k]
        return where

    def free_range(gen, axis, msub=None):
        _, m_lo, mn, par = GENS[gen]
        if axis == "z":
            return (m_lo, mn) if msub is None else (msub, 1)
        if axis == "y" and par is not None:
            return 2 * par, 2
        return 0, 4

    def copy_of(gen, part, phase, kind, msub=None):
        h, step, b, direction = KINDS[kind]
        g = GENS[gen][0]
        gsl = pl.ds(0, 2) if g is None else pl.ds(g, 1)
        row0, nr = PART_ROWS[part]
        where, land = place(part, phase, step), [gsl, h]
        for a in AXES:
            if a not in where:
                where[a] = pl.ds(*free_range(gen, a, msub))
                land.append(where[a])
        src = acc.at[(gsl, h, where["z"], where["y"], where["x"], pl.ds(row0, nr), slice(None))]
        return remote((gen, part, phase, kind), src, hop_bufs[part, phase][b].at[tuple(land)],
                      device(ORDER[part][phase], direction))

    def send(gen, part, phase, kind):
        cond = active(gen, part, phase, KINDS[kind][1])
        copy = copy_of(gen, part, phase, kind)
        when(cond, copy.start)
        sent.append((copy, cond))

    def ring_start(gen, kinds, m=None):
        last = m is None or m == 2
        for kind in kinds:
            for part in (1, 2, 0):
                step = KINDS[kind][1]
                cond = active(gen, part, 0, step)
                if ORDER[part][0] == "z":
                    copy = copy_of(gen, part, 0, kind)
                    when(at["z"][step] == (3 if m is None else m), copy.start)
                else:
                    copy = copy_of(gen, part, 0, kind, m)
                    when(cond, copy.start)
                if last:
                    sent.append((copy_of(gen, part, 0, kind), cond))

    def add_into(gen, part, phase, hs, step, bufs):
        row0, nr = PART_ROWS[part]
        g = GENS[gen][0]
        where, land = place(part, phase, step), []
        for a in AXES:
            if a not in where:
                where[a] = pl.ds(*free_range(gen, a))
                land.append(where[a])
        for gi in ((0, 1) if g is None else (g,)):
            for h in hs:
                spot = (gi, h, where["z"], where["y"], where["x"], pl.ds(row0, nr), slice(None))
                total = acc[spot]
                for b in bufs:
                    total = total + b[(gi, h, *land, slice(None), slice(None))]
                acc[spot] = total

    def relay(gens, phase, parts=(1, 2, 0)):
        for part in parts:
            for gen in gens:
                for got, out in (("1A", "RA"), ("1B", "LB")):
                    step = KINDS[out][1]
                    cond = active(gen, part, phase, step)
                    arrived = copy_of(gen, part, phase, got)
                    copy = copy_of(gen, part, phase, out)

                    def go():
                        arrived.wait_recv()
                        add_into(gen, part, phase, (KINDS[out][0],), step, [hop_bufs[part, phase][0]])
                        copy.start()

                    when(cond, go)
                    sent.append((copy, cond))

    def finish(gens, phase, parts=(1, 2, 0)):
        for part in parts:
            for gen in gens:
                arrivals = [copy_of(gen, part, phase, k) for k in (LAST if phase == 2 else RING)]

                def go():
                    for a in arrivals:
                        a.wait_recv()
                    add_into(gen, part, phase, (0, 1), 0, list(hop_bufs[part, phase][0 if phase == 2 else 1:]))

                when(active(gen, part, phase, 0), go)
                if phase < 2:
                    for kind in (RAW if phase == 0 else LAST):
                        send(gen, part, phase + 1, kind)

    def wait_sends(copies):
        for copy, cond in copies:
            when(cond, copy.wait_send)
        copies.clear()

    own0 = pl.multiple_of(core * TOK, TOK)
    oth0 = pl.multiple_of(other * TOK, TOK)
    barrier = pltpu.get_barrier_semaphore()
    for dev in [partner] + [device(a, s) for a in AXES for s in (1, -1)]:
        pl.semaphore_signal(barrier, inc=1, device_id=dev, device_id_type=MESH)
    own_c = pl.ds(pl.multiple_of(core * HALF, HALF), HALF)
    oth_c = pl.ds(pl.multiple_of(other * HALF, HALF), HALF)
    loads = {}

    def load(name, src, dst):
        loads[name] = pltpu.make_async_copy(src, dst, local_sem.at[len(loads)])
        loads[name].start()

    load("x", x_hbm, xf.at[pl.ds(own0, TOK)])
    for name, src, dst in (("wq", wq_hbm, wq), ("wk", wk_hbm, wk), ("wv", wv_hbm, wv)):
        load(name, src.at[:, own_c], dst)
    load("dy", dy_hbm, dyf.at[pl.ds(own0, TOK)])
    load("wo", wo_hbm.at[own_c], wo)

    lanes = lax.broadcasted_iota(jnp.int32, (1, 128), 1)
    first = (lanes < 64).astype(F32).astype(BF16)
    second = (lanes >= 64).astype(F32).astype(BF16)
    causal = (lax.broadcasted_iota(jnp.int32, (CHUNK, CHUNK), 0)
              >= lax.broadcasted_iota(jnp.int32, (CHUNK, CHUNK), 1))
    block_diag = ((lax.broadcasted_iota(jnp.int32, (128, 128), 0) < 64)
                  == (lax.broadcasted_iota(jnp.int32, (128, 128), 1) < 64))

    def chunk_products(a, b, raw, base, blk):
        for n in range(blk // CHUNK):
            rs = slice(n * CHUNK, (n + 1) * CHUNK)
            p = t_dot(a[rs, :], b[rs, :])
            for j in range(2):
                cs = slice(j * 128, j * 128 + 128)
                raw[lax.div(base, CHUNK) + n, j] = p[cs, cs]

    def project_x(g, base, blk):
        rows = pl.ds(base, blk)
        gcols = pl.ds(g * GRP, GRP)
        xa = xf[rows, :]
        if g == 0:
            xt[:, rows] = xa.T
        kept = []
        for w, sg, out in ((wq, sga, qg), (wk, sgb, kg)):
            a = dot(xa, w[:, gcols])
            s = pl.reciprocal(1.0 + jnp.exp(-a))
            kept.append((a * s).astype(BF16))
            out[rows, :] = kept[-1]
            sg[rows, :] = s * (1.0 + a * (1.0 - s))
        v = dot(xa, wv[:, gcols]).astype(BF16)
        vg[rows, :] = v
        chunk_products(kept[1], v, kv_raw, base, blk)

    def project_dy(g, half, base):
        rows = pl.ds(base, TOK)
        do = dot_t(dyf[rows, :], wo[pl.ds(g * GRP, GRP), :]).astype(BF16)
        dx_ref[:, pl.ds(pl.multiple_of(half * GRP, GRP), GRP)] = do
        chunk_products(qg[rows, :], do, qd_raw, base, TOK)

    def scan_states():
        for raw, side, order in ((kv_raw, 0, range(NCH)), (qd_raw, 1, range(NCH - 1, -1, -1))):
            for j in range(2):
                st = jnp.zeros((128, 128), F32)
                for i in order:
                    y_ref[i * 128:i * 128 + 128, (side * 2 + j) * 128:(side * 2 + j) * 128 + 128] = st.astype(BF16)
                    st = st + jnp.where(block_diag, raw[i, j], 0.0)

    def attend(g, lo, hi):
        def body(i, _):
            rows = pl.ds(pl.multiple_of(i * CHUNK, CHUNK), CHUNK)
            srows = pl.ds(pl.multiple_of(i * 128, 128), 128)
            drows = pl.ds(pl.multiple_of(lax.rem(i, 4) * CHUNK, CHUNK), CHUNK)
            for j in range(2):
                cols = pl.ds(j * 128, 128)
                pre, suf = y_ref[srows, cols], y_ref[srows, pl.ds(256 + j * 128, 128)]
                ocols = pl.ds(g * GRP + j * 128, 128)
                q, k, v = qg[rows, cols], kg[rows, cols], vg[rows, cols]
                do = dx_ref[drows, pl.ds(pl.multiple_of(lax.div(i, 4) * GRP + j * 128, 128), 128)]
                qa, qb, ka, kb = q * first, q * second, k * first, k * second
                va, vb, da, db = v * first, v * second, do * first, do * second
                p_a = jnp.where(causal, dot_t(qa, k), 0.0).astype(BF16)
                p_b = jnp.where(causal, dot_t(qb, k), 0.0).astype(BF16)
                d_a = jnp.where(causal, dot_t(da, v), 0.0).astype(BF16)
                d_b = jnp.where(causal, dot_t(db, v), 0.0).astype(BF16)
                o = dot(p_a, va) + dot(p_b, vb) + dot(q, pre)
                oo[rows, ocols] = (scale * o).astype(BF16)
                dq = dot(d_a, ka) + dot(d_b, kb) + dot_t(do, pre)
                gq[rows, ocols] = (scale * dq * sga[rows, cols]).astype(BF16)
                dk = t_dot(d_a, qa) + t_dot(d_b, qb) + dot_t(v, suf)
                gk[rows, ocols] = (scale * dk * sgb[rows, cols]).astype(BF16)
                dv = t_dot(p_a, da) + t_dot(p_b, db) + dot(k, suf)
                gv[rows, ocols] = (scale * dv).astype(BF16)
            return 0

        lax.fori_loop(lo, hi, body, 0)

    def weight_grad(g, m):
        gr = (gq, gk, gv)[m]

        for n in range(2):
            t = dot(xt[n * 512:n * 512 + 512, :], gr[:, pl.ds(g * GRP, GRP)])
            for h in range(2):
                for yy in range(2):
                    for xx in range(4):
                        r = yy * 256 + xx * 64
                        acc[g, h, m, yy * 2 + n, xx] = t[r:r + 64, h * 128:h * 128 + 128]

    def out_weight_grad(g):
        rhs_cols = pl.ds(pl.multiple_of(core * HALF, HALF), HALF)
        for src, who in ((oo, core), (o_in, other)):
            t = t_dot(src[:, pl.ds(g * GRP, GRP)], dyf[:, rhs_cols])
            for gg in range(2):
                for h in range(2):
                    for xx in range(4):
                        c0 = gg * 256 + h * 128
                        acc[gg, h, 3, g * 2 + who, xx] = t[xx * 64:xx * 64 + 64, c0:c0 + 128]

    def share(g):
        cols = pl.ds(g * GRP, GRP)
        o_copy = remote(("o", g), oo.at[:, cols], o_in.at[:, cols], partner)
        start(o_copy)
        g_copies = []
        for m, gr in enumerate((gq, gk, gv)):
            g_copies.append(remote(("g", g, m), gr.at[pl.ds(oth0, TOK), cols], g_in.at[m, :, cols], partner))
            start(g_copies[-1])
        return o_copy, g_copies

    a0 = core * TOK
    with jax.named_scope("load0"):
        for name in ("x", "wq", "wk", "wv"):
            loads[name].wait()
    project_x(0, pl.multiple_of(a0, BLK), BLK)
    with jax.named_scope("barrier"):
        pl.semaphore_wait(barrier, 7)
    x_send = remote("x", x_hbm, xf.at[pl.ds(own0, TOK)], partner)
    dy_send = remote("dy", dy_hbm, dyf.at[pl.ds(own0, TOK)], partner)
    start(x_send)
    start(dy_send)
    with jax.named_scope("projA0"):
        project_x(0, pl.multiple_of(a0 + BLK, BLK), BLK)
        for name in ("dy", "wo"):
            loads[name].wait()
        project_dy(0, core, own0)
    with jax.named_scope("xrecv"):
        x_send.wait_recv()
    with jax.named_scope("projB0"):
        for n in range(2):
            project_x(0, pl.multiple_of(oth0 + n * BLK, BLK), BLK)
    with jax.named_scope("dyrecv"):
        dy_send.wait_recv()
    with jax.named_scope("projBd0"):
        project_dy(0, other, oth0)
    with jax.named_scope("scan0"):
        scan_states()
    with jax.named_scope("attend0"):
        attend(0, 0, NCH)
    o_copy0, g_copies0 = share(0)
    with jax.named_scope("wgrad0"):
        for m in range(3):
            weight_grad(0, m)
            ring_start("E0", ("1A", "1B"), m)
    with jax.named_scope("dwo0"):
        o_copy0.wait_recv()
        out_weight_grad(0)
        ring_start("L0", ("1A", "1B"))
        for m in range(3):
            ring_start("E0", ("RB", "LA"), m)
        ring_start("L0", ("RB", "LA"))

    with jax.named_scope("projA1"):
        for n in range(2):
            project_x(1, pl.multiple_of(own0 + n * BLK, BLK), BLK)
        project_dy(1, core, own0)
    with jax.named_scope("r1E0"):
        relay(("E0",), 0)
    with jax.named_scope("projB1a"):
        for n in range(2):
            project_x(1, pl.multiple_of(oth0 + n * BLK, BLK), BLK)
    with jax.named_scope("r1L0"):
        relay(("L0",), 0)
    with jax.named_scope("projB1b"):
        project_dy(1, other, oth0)
    load("wq2", wq_hbm.at[:, oth_c], xf.at[pl.ds(0, DIM), pl.ds(0, HALF)])
    load("wk2", wk_hbm.at[:, oth_c], xf.at[pl.ds(0, DIM), pl.ds(HALF, HALF)])
    load("wv2", wv_hbm.at[:, oth_c], xf.at[pl.ds(DIM, DIM), pl.ds(0, HALF)])
    for n in range(2):
        load(f"wo2{n}", wo_hbm.at[oth_c, pl.ds(n * HALF, HALF)], xf.at[pl.ds(DIM + n * HALF, HALF), pl.ds(HALF, HALF)])
    with jax.named_scope("scan1"):
        scan_states()
    with jax.named_scope("attend1a"):
        attend(1, 0, 3)
    with jax.named_scope("f1_0"):
        finish(("E0", "L0"), 0)
    with jax.named_scope("attend1b"):
        attend(1, 3, 7)
    with jax.named_scope("r2_0"):
        relay(("E0", "L0"), 1)
    with jax.named_scope("attend1c"):
        attend(1, 7, 8)
    o_copy1, g_copies1 = share(1)
    with jax.named_scope("wgrad1"):
        for m in range(3):
            weight_grad(1, m)
            ring_start("E1", ("1A", "1B"), m)
            if m == 1:
                with jax.named_scope("f2_0"):
                    finish(("E0", "L0"), 1)
    with jax.named_scope("dwo1"):
        o_copy1.wait_recv()
        out_weight_grad(1)
        ring_start("L1", ("1A", "1B"))
        for m in range(3):
            ring_start("E1", ("RB", "LA"), m)
        ring_start("L1", ("RB", "LA"))

    def y_part(r, n):
        rows, cols = pl.ds(pl.multiple_of(own0 + r * HALF, HALF), HALF), pl.ds(n * HALF, HALF)
        t = dot(oo[rows, :], wo[:, cols]) + dot(o_in[rows, :], xf[pl.ds(DIM + n * HALF, HALF), pl.ds(HALF, HALF)])
        y_ref[pl.ds(r * HALF, HALF), cols] = t.astype(BF16)

    def dx_part(r, n):
        rows, cols = pl.ds(pl.multiple_of(own0 + r * HALF, HALF), HALF), pl.ds(n * HALF, HALF)
        t = None
        for m, (gr, w, w2) in enumerate(((gq, wq, xf.at[cols, pl.ds(0, HALF)]), (gk, wk, xf.at[cols, pl.ds(HALF, HALF)]),
                                         (gv, wv, xf.at[pl.ds(DIM + n * HALF, HALF), pl.ds(0, HALF)]))):
            u = dot_t(gr[rows, :], w[cols, :]) + dot_t(g_in[m, pl.ds(r * HALF, HALF), :], w2[...])
            t = u if t is None else t + u
        dx_ref[pl.ds(r * HALF, HALF), cols] = t.astype(BF16)

    for name in ("wq2", "wk2", "wv2", "wo20", "wo21"):
        loads[name].wait()
    with jax.named_scope("Y"):
        for r in range(2):
            for n in range(2):
                y_part(r, n)
    for c in g_copies0 + g_copies1:
        c.wait_recv()
    with jax.named_scope("dX0"):
        dx_part(0, 0)
    with jax.named_scope("r1E1"):
        relay(("E1", "L1"), 0)
    with jax.named_scope("dX1"):
        dx_part(0, 1)
    with jax.named_scope("f3_0"):
        finish(("E0", "L0"), 2)
    with jax.named_scope("dX2"):
        dx_part(1, 0)
    with jax.named_scope("dX3"):
        dx_part(1, 1)
    last_gens = ("E1", "L1")
    with jax.named_scope("f1_1"):
        finish(last_gens, 0)
    with jax.named_scope("sends"):
        early = sent[:-36]
        del sent[:-36]
        wait_sends(early)
    with jax.named_scope("r2_1"):
        relay(last_gens, 1)
    with jax.named_scope("f2_1"):
        finish(last_gens, 1)
    with jax.named_scope("f3_1"):
        finish(last_gens, 2)

    final = acc.at[:, :, me["z"], yat[0], me["x"]]
    last = remote("final", final, fin, partner)
    start(last)
    with jax.named_scope("sends2"):
        for g in range(2):
            for h in range(2):
                cols = pl.ds(pl.multiple_of(core * HALF + g * 256 + h * 128, 128), 128)
                dw_ref[:, cols] = acc[g, h, me["z"], yat[0], me["x"]]
        wait_sends(sent)
    with jax.named_scope("last"):
        last.wait_recv()
    for g in range(2):
        for h in range(2):
            cols = pl.ds(pl.multiple_of(other * HALF + g * 256 + h * 128, 128), 128)
            dw_ref[:, cols] = fin[g, h]
    wait_sends(sent)


def hop_shapes(part, phase):
    rest = 2 - phase
    return [pltpu.VMEM((2, 2) + (4,) * rest + (PART_ROWS[part][1], 128), F32)] * 3


def solution(mesh):
    act = P(("pod", "data"), "seq", None)
    scale = float((64 * SEQ) ** -0.5)

    def local(x, wq, wk, wv, wo, dy):
        vm = pltpu.VMEM
        any_ = pl.BlockSpec(memory_space=pl.ANY)
        scratch = [
            vm((SEQ, DIM), BF16), vm((DIM, SEQ), BF16), vm((SEQ, DIM), BF16),
            *[vm((DIM, HALF), BF16)] * 3, vm((HALF, DIM), BF16),
            *[vm((SEQ, GRP), F32)] * 2, *[vm((SEQ, GRP), BF16)] * 3,
            *[vm((NCH, 2, 128, 128), F32)] * 2,
            vm((SEQ, HALF), BF16), vm((SEQ, HALF), BF16), *[vm((SEQ, HALF), BF16)] * 3, vm((3, TOK, HALF), BF16),
            vm((2, 2, 4, 4, 4, ROWS, 128), F32), vm((2, 2, ROWS, 128), F32),
        ]
        for part in range(3):
            for phase in range(3):
                scratch += hop_shapes(part, phase)
        scratch += [pltpu.SemaphoreType.DMA((NUM_SEMS,)), pltpu.SemaphoreType.DMA((NUM_SEMS,)),
                    pltpu.SemaphoreType.DMA((NUM_LOCAL,))]
        y, dx, dw = pl.pallas_call(
            lambda *refs: kernel(scale, *refs),
            out_shape=(vm((TOK, DIM), BF16), vm((TOK, DIM), BF16), vm((ROWS, DIM), F32)),
            in_specs=[any_] * 6,
            out_specs=(pl.BlockSpec(memory_space=pltpu.VMEM),) * 3,
            scratch_shapes=scratch,
            name="layer",
            compiler_params=pltpu.CompilerParams(collective_id=0, has_side_effects=True, vmem_limit_bytes=62560000),
        )(x[0], dy[0], wq, wk, wv, wo.reshape(DIM, DIM))
        return y[None], dx[None], dw

    return jax.shard_map(local, mesh=mesh,
                         in_specs=(act, P(None, None), P(None, None), P(None, None), P(None, None, None), act),
                         out_specs=(act, act, P(("pod", "data"), None)), check_vma=False)
```

```python
import jax
import jax.numpy as jnp
from jax import lax
from jax.experimental import pallas as pl
from jax.experimental.pallas import tpu as pltpu
from jax.sharding import PartitionSpec as P

MESH = pl.DeviceIdType.MESH
F32 = jnp.float32
BF16 = jnp.bfloat16

TOK = 1024
SEQ = 2 * TOK
DIM = 1024
HALF = DIM // 2
GRP = 256
CHUNK = 256
NCH = SEQ // CHUNK
BLK = 512
ROWS = 64

ORDER = (("z", "y", "x"), ("y", "x", "z"), ("x", "z", "y"))
PART_ROWS = ((0, 16), (16, 24), (40, 24))
AXES = ("z", "y", "x")


def dot(a, b):
    return lax.dot_general(a, b, (((1,), (0,)), ((), ())), preferred_element_type=F32)


def dot_t(a, b):
    return lax.dot_general(a, b, (((1,), (1,)), ((), ())), preferred_element_type=F32)


def t_dot(a, b):
    return lax.dot_general(a, b, (((0,), (0,)), ((), ())), preferred_element_type=F32)


NUM_SEMS = 240
NUM_LOCAL = 12
KINDS = {"1A": (0, 2, 0, 1), "1B": (1, 2, 0, -1), "RB": (1, 1, 1, 1), "LA": (0, 3, 2, -1),
         "RA": (0, 1, 1, 1), "LB": (1, 3, 2, -1),
         "O": (slice(None), 2, 0, 2), "R": (slice(None), 1, 1, 1), "L": (slice(None), 3, 2, -1)}
RAW = ("1A", "1B", "RB", "LA")
RING = ("RB", "LA", "RA", "LB")
LAST = ("O", "R", "L")
GENS = {"E0": (0, 0, 3, None), "L0": (None, 3, 1, 0), "E1": (1, 0, 3, None), "L1": (None, 3, 1, 1)}


def when(cond, fn):
    if cond is None:
        fn()
    else:
        pl.when(cond)(fn)


def both(a, b):
    return b if a is None else a if b is None else jnp.logical_and(a, b)


def kernel(scale, x_hbm, dy_hbm, wq_hbm, wk_hbm, wv_hbm, wo_hbm,
           y_ref, dx_ref, dw_ref,
           xf, xt, dyf, wq, wk, wv, wo, sga, sgb, qg, kg, vg,
           kv_raw, qd_raw, oo, o_in, gq, gk, gv, g_in, acc, fin,
           r00, l00, m00, r01, l01, m01, r02, l02, m02,
           r10, l10, m10, r11, l11, m11, r12, l12, m12,
           r20, l20, m20, r21, l21, m21, r22, l22, m22,
           send_sem, recv_sem, local_sem):
    core = lax.axis_index("seq")
    data = lax.axis_index("data")
    me = {"z": lax.div(data, 16), "y": lax.rem(lax.div(data, 4), 4), "x": lax.rem(data, 4)}
    at = {a: [me[a]] + [lax.rem(me[a] + k, 4) for k in (1, 2, 3)] for a in AXES}
    yat = [lax.rem(v, 2) * 2 + lax.div(v, 2) for v in at["y"]]
    stride = {"z": 16, "y": 4, "x": 1}
    away = {a: [data + (at[a][k] - me[a]) * stride[a] for k in range(4)] for a in AXES}
    is_last = [v == 3 for v in at["z"]]
    not_last = [v != 3 for v in at["z"]]
    parity = [[lax.rem(v, 2) == par for v in at["y"]] for par in (0, 1)]
    conds = {}
    other = 1 - core
    hop_bufs = {(0, 0): (r00, l00, m00), (0, 1): (r01, l01, m01), (0, 2): (r02, l02, m02),
                (1, 0): (r10, l10, m10), (1, 1): (r11, l11, m11), (1, 2): (r12, l12, m12),
                (2, 0): (r20, l20, m20), (2, 1): (r21, l21, m21), (2, 2): (r22, l22, m22)}
    sem_ids = {}
    sent = []

    def device(axis, delta):
        return {"data": away[axis][delta % 4], "seq": core}

    partner = {"data": data, "seq": other}

    def remote(name, src, dst, dev):
        k = sem_ids.setdefault(name, len(sem_ids))
        assert k < NUM_SEMS
        return pltpu.make_async_remote_copy(src_ref=src, dst_ref=dst, send_sem=send_sem.at[k],
                                            recv_sem=recv_sem.at[k], device_id=dev, device_id_type=MESH)

    def start(copy):
        copy.start()
        sent.append((copy, None))

    def gen_test(gen, axis, k):
        _, m_lo, _, par = GENS[gen]
        if axis == "z":
            return ("z", m_lo != 0, k)
        if axis == "y" and par is not None:
            return ("y", par, k)
        return None

    def active(gen, part, phase, step):
        tests = [gen_test(gen, axis, 0 if p < phase else step) for p, axis in enumerate(ORDER[part][:phase + 1])]
        key = tuple(sorted(t for t in tests if t is not None))
        if key not in conds:
            cond = None
            for axis, kind, k in key:
                cond = both(cond, (is_last if kind else not_last)[k] if axis == "z" else parity[kind][k])
            conds[key] = cond
        return conds[key]

    def place(part, phase, step):
        where = {}
        for p, a in enumerate(ORDER[part][:phase + 1]):
            k = 0 if p < phase else step
            where[a] = yat[k] if a == "y" else at[a][k]
        return where

    def free_range(gen, axis, msub=None):
        _, m_lo, mn, par = GENS[gen]
        if axis == "z":
            return (m_lo, mn) if msub is None else (msub, 1)
        if axis == "y" and par is not None:
            return 2 * par, 2
        return 0, 4

    def copy_of(gen, part, phase, kind, msub=None):
        h, step, b, direction = KINDS[kind]
        g = GENS[gen][0]
        gsl = pl.ds(0, 2) if g is None else pl.ds(g, 1)
        row0, nr = PART_ROWS[part]
        where, land = place(part, phase, step), [gsl, h]
        for a in AXES:
            if a not in where:
                where[a] = pl.ds(*free_range(gen, a, msub))
                land.append(where[a])
        src = acc.at[(gsl, h, where["z"], where["y"], where["x"], pl.ds(row0, nr), slice(None))]
        return remote((gen, part, phase, kind), src, hop_bufs[part, phase][b].at[tuple(land)],
                      device(ORDER[part][phase], direction))

    def send(gen, part, phase, kind):
        cond = active(gen, part, phase, KINDS[kind][1])
        copy = copy_of(gen, part, phase, kind)
        when(cond, copy.start)
        sent.append((copy, cond))

    def ring_start(gen, kinds, m=None):
        last = m is None or m == 2
        for kind in kinds:
            for part in (1, 2, 0):
                step = KINDS[kind][1]
                cond = active(gen, part, 0, step)
                if ORDER[part][0] == "z":
                    copy = copy_of(gen, part, 0, kind)
                    when(at["z"][step] == (3 if m is None else m), copy.start)
                else:
                    copy = copy_of(gen, part, 0, kind, m)
                    when(cond, copy.start)
                if last:
                    sent.append((copy_of(gen, part, 0, kind), cond))

    def add_into(gen, part, phase, hs, step, bufs):
        row0, nr = PART_ROWS[part]
        g = GENS[gen][0]
        where, land = place(part, phase, step), []
        for a in AXES:
            if a not in where:
                where[a] = pl.ds(*free_range(gen, a))
                land.append(where[a])
        for gi in ((0, 1) if g is None else (g,)):
            for h in hs:
                spot = (gi, h, where["z"], where["y"], where["x"], pl.ds(row0, nr), slice(None))
                total = acc[spot]
                for b in bufs:
                    total = total + b[(gi, h, *land, slice(None), slice(None))]
                acc[spot] = total

    def relay(gens, phase, parts=(1, 2, 0)):
        for part in parts:
            for gen in gens:
                for got, out in (("1A", "RA"), ("1B", "LB")):
                    step = KINDS[out][1]
                    cond = active(gen, part, phase, step)
                    arrived = copy_of(gen, part, phase, got)
                    copy = copy_of(gen, part, phase, out)

                    def go():
                        arrived.wait_recv()
                        add_into(gen, part, phase, (KINDS[out][0],), step, [hop_bufs[part, phase][0]])
                        copy.start()

                    when(cond, go)
                    sent.append((copy, cond))

    def finish(gens, phase, parts=(1, 2, 0)):
        for part in parts:
            for gen in gens:
                arrivals = [copy_of(gen, part, phase, k) for k in (LAST if phase == 2 else RING)]

                def go():
                    for a in arrivals:
                        a.wait_recv()
                    add_into(gen, part, phase, (0, 1), 0, list(hop_bufs[part, phase][0 if phase == 2 else 1:]))

                when(active(gen, part, phase, 0), go)
                if phase < 2:
                    for kind in (RAW if phase == 0 else LAST):
                        send(gen, part, phase + 1, kind)

    def wait_sends(copies):
        for copy, cond in copies:
            when(cond, copy.wait_send)
        copies.clear()

    own0 = pl.multiple_of(core * TOK, TOK)
    oth0 = pl.multiple_of(other * TOK, TOK)
    barrier = pltpu.get_barrier_semaphore()
    for dev in [partner] + [device(a, s) for a in AXES for s in (1, -1)]:
        pl.semaphore_signal(barrier, inc=1, device_id=dev, device_id_type=MESH)
    own_c = pl.ds(pl.multiple_of(core * HALF, HALF), HALF)
    oth_c = pl.ds(pl.multiple_of(other * HALF, HALF), HALF)
    loads = {}

    def load(name, src, dst):
        loads[name] = pltpu.make_async_copy(src, dst, local_sem.at[len(loads)])
        loads[name].start()

    load("x", x_hbm, xf.at[pl.ds(own0, TOK)])
    for name, src, dst in (("wq", wq_hbm, wq), ("wk", wk_hbm, wk), ("wv", wv_hbm, wv)):
        load(name, src.at[:, own_c], dst)
    load("dy", dy_hbm, dyf.at[pl.ds(own0, TOK)])
    load("wo", wo_hbm.at[own_c], wo)

    lanes = lax.broadcasted_iota(jnp.int32, (1, 128), 1)
    first = (lanes < 64).astype(F32).astype(BF16)
    second = (lanes >= 64).astype(F32).astype(BF16)
    tri = (lax.broadcasted_iota(jnp.int32, (128, 256), 0)
           >= lax.rem(lax.broadcasted_iota(jnp.int32, (128, 256), 1), 128))

    def stacked(a, n):
        part = a[n * 128:n * 128 + 128]
        return jnp.concatenate([part * first, part * second], axis=0)

    def masked(sc):
        top = jnp.where(tri, sc[:128], 0.0).astype(BF16)
        return top if sc.shape[0] == 128 else jnp.concatenate([top, sc[128:].astype(BF16)], axis=0)

    def lower(full, extra):
        return jnp.concatenate([full[:128], full[128:] + extra], axis=0)

    def turned(s0, s1, r):
        wide = t_dot(s0, r)
        tail = jnp.concatenate([s1[:, :128].T, s1[:, 128:].T], axis=1)
        return jnp.concatenate([jnp.where(lanes < 64, wide[:128], wide[128:]), dot(tail, stacked(r, 1))], axis=0)

    block_diag = ((lax.broadcasted_iota(jnp.int32, (128, 128), 0) < 64)
                  == (lax.broadcasted_iota(jnp.int32, (128, 128), 1) < 64))

    def chunk_products(a, b, raw, base, blk):
        for n in range(blk // CHUNK):
            rs = slice(n * CHUNK, (n + 1) * CHUNK)
            p = t_dot(a[rs, :], b[rs, :])
            for j in range(2):
                cs = slice(j * 128, j * 128 + 128)
                raw[lax.div(base, CHUNK) + n, j] = p[cs, cs]

    def project_x(g, base, blk):
        rows = pl.ds(base, blk)
        gcols = pl.ds(g * GRP, GRP)
        xa = xf[rows, :]
        if g == 0:
            xt[:, rows] = xa.T
        kept = []
        for w, sg, out in ((wq, sga, qg), (wk, sgb, kg)):
            a = dot(xa, w[:, gcols])
            s = pl.reciprocal(1.0 + jnp.exp(-a))
            kept.append((a * s).astype(BF16))
            out[rows, :] = kept[-1]
            sg[rows, :] = s * (1.0 + a * (1.0 - s))
        v = dot(xa, wv[:, gcols]).astype(BF16)
        vg[rows, :] = v
        chunk_products(kept[1], v, kv_raw, base, blk)

    def project_dy(g, half, base):
        rows = pl.ds(base, TOK)
        do = dot_t(dyf[rows, :], wo[pl.ds(g * GRP, GRP), :]).astype(BF16)
        dx_ref[:, pl.ds(pl.multiple_of(half * GRP, GRP), GRP)] = do
        chunk_products(qg[rows, :], do, qd_raw, base, TOK)

    def scan_states():
        for raw, side, order in ((kv_raw, 0, range(NCH)), (qd_raw, 1, range(NCH - 1, -1, -1))):
            for j in range(2):
                st = jnp.zeros((128, 128), F32)
                for i in order:
                    y_ref[i * 128:i * 128 + 128, (side * 2 + j) * 128:(side * 2 + j) * 128 + 128] = st.astype(BF16)
                    st = st + jnp.where(block_diag, raw[i, j], 0.0)

    def attend(g, lo, hi):
        def body(i, _):
            rows = pl.ds(pl.multiple_of(i * CHUNK, CHUNK), CHUNK)
            srows = pl.ds(pl.multiple_of(i * 128, 128), 128)
            drows = pl.ds(pl.multiple_of(lax.rem(i, 4) * CHUNK, CHUNK), CHUNK)
            for j in range(2):
                cols = pl.ds(j * 128, 128)
                pre, suf = y_ref[srows, cols], y_ref[srows, pl.ds(256 + j * 128, 128)]
                ocols = pl.ds(g * GRP + j * 128, 128)
                q, k, v = qg[rows, cols], kg[rows, cols], vg[rows, cols]
                do = dx_ref[drows, pl.ds(pl.multiple_of(lax.div(i, 4) * GRP + j * 128, 128), 128)]
                k0, k1, v0, v1 = stacked(k, 0), stacked(k, 1), stacked(v, 0), stacked(v, 1)
                p0, p1 = masked(dot_t(q, k0)), masked(dot_t(q[128:], k1))
                d0, d1 = masked(dot_t(do, v0)), masked(dot_t(do[128:], v1))
                o = lower(dot(p0, v0) + dot(q, pre), dot(p1, v1))
                oo[rows, ocols] = (scale * o).astype(BF16)
                dq = lower(dot(d0, k0) + dot_t(do, pre), dot(d1, k1))
                gq[rows, ocols] = (scale * dq * sga[rows, cols]).astype(BF16)
                dk = dot_t(v, suf) + turned(d0, d1, q)
                gk[rows, ocols] = (scale * dk * sgb[rows, cols]).astype(BF16)
                dv = dot(k, suf) + turned(p0, p1, do)
                gv[rows, ocols] = (scale * dv).astype(BF16)
            return 0

        lax.fori_loop(lo, hi, body, 0)

    def weight_grad(g, m):
        gr = (gq, gk, gv)[m]

        for n in range(2):
            t = dot(xt[n * 512:n * 512 + 512, :], gr[:, pl.ds(g * GRP, GRP)])
            for h in range(2):
                for yy in range(2):
                    for xx in range(4):
                        r = yy * 256 + xx * 64
                        acc[g, h, m, yy * 2 + n, xx] = t[r:r + 64, h * 128:h * 128 + 128]

    def out_weight_grad(g):
        rhs_cols = pl.ds(pl.multiple_of(core * HALF, HALF), HALF)
        for src, who in ((oo, core), (o_in, other)):
            t = t_dot(src[:, pl.ds(g * GRP, GRP)], dyf[:, rhs_cols])
            for gg in range(2):
                for h in range(2):
                    for xx in range(4):
                        c0 = gg * 256 + h * 128
                        acc[gg, h, 3, g * 2 + who, xx] = t[xx * 64:xx * 64 + 64, c0:c0 + 128]

    def share(g):
        cols = pl.ds(g * GRP, GRP)
        o_copy = remote(("o", g), oo.at[:, cols], o_in.at[:, cols], partner)
        start(o_copy)
        g_copies = []
        for m, gr in enumerate((gq, gk, gv)):
            g_copies.append(remote(("g", g, m), gr.at[pl.ds(oth0, TOK), cols], g_in.at[m, :, cols], partner))
            start(g_copies[-1])
        return o_copy, g_copies

    a0 = core * TOK
    with jax.named_scope("load0"):
        for name in ("x", "wq", "wk", "wv"):
            loads[name].wait()
    project_x(0, pl.multiple_of(a0, BLK), BLK)
    with jax.named_scope("barrier"):
        pl.semaphore_wait(barrier, 7)
    x_send = remote("x", x_hbm, xf.at[pl.ds(own0, TOK)], partner)
    dy_send = remote("dy", dy_hbm, dyf.at[pl.ds(own0, TOK)], partner)
    start(x_send)
    start(dy_send)
    with jax.named_scope("projA0"):
        project_x(0, pl.multiple_of(a0 + BLK, BLK), BLK)
        for name in ("dy", "wo"):
            loads[name].wait()
        project_dy(0, core, own0)
    with jax.named_scope("xrecv"):
        x_send.wait_recv()
    with jax.named_scope("projB0"):
        for n in range(2):
            project_x(0, pl.multiple_of(oth0 + n * BLK, BLK), BLK)
    with jax.named_scope("dyrecv"):
        dy_send.wait_recv()
    with jax.named_scope("projBd0"):
        project_dy(0, other, oth0)
    with jax.named_scope("scan0"):
        scan_states()
    with jax.named_scope("attend0"):
        attend(0, 0, NCH)
    o_copy0, g_copies0 = share(0)
    with jax.named_scope("wgrad0"):
        for m in range(3):
            weight_grad(0, m)
            ring_start("E0", ("1A", "1B"), m)
    with jax.named_scope("dwo0"):
        o_copy0.wait_recv()
        out_weight_grad(0)
        ring_start("L0", ("1A", "1B"))
        for m in range(3):
            ring_start("E0", ("RB", "LA"), m)
        ring_start("L0", ("RB", "LA"))

    with jax.named_scope("projA1"):
        for n in range(2):
            project_x(1, pl.multiple_of(own0 + n * BLK, BLK), BLK)
        project_dy(1, core, own0)
    with jax.named_scope("r1E0"):
        relay(("E0",), 0)
    with jax.named_scope("projB1a"):
        for n in range(2):
            project_x(1, pl.multiple_of(oth0 + n * BLK, BLK), BLK)
    with jax.named_scope("r1L0"):
        relay(("L0",), 0)
    with jax.named_scope("projB1b"):
        project_dy(1, other, oth0)
    load("wq2", wq_hbm.at[:, oth_c], xf.at[pl.ds(0, DIM), pl.ds(0, HALF)])
    load("wk2", wk_hbm.at[:, oth_c], xf.at[pl.ds(0, DIM), pl.ds(HALF, HALF)])
    load("wv2", wv_hbm.at[:, oth_c], xf.at[pl.ds(DIM, DIM), pl.ds(0, HALF)])
    for n in range(2):
        load(f"wo2{n}", wo_hbm.at[oth_c, pl.ds(n * HALF, HALF)], xf.at[pl.ds(DIM + n * HALF, HALF), pl.ds(HALF, HALF)])
    with jax.named_scope("scan1"):
        scan_states()
    with jax.named_scope("attend1a"):
        attend(1, 0, 3)
    with jax.named_scope("f1_0"):
        finish(("E0", "L0"), 0)
    with jax.named_scope("attend1b"):
        attend(1, 3, 7)
    with jax.named_scope("r2_0"):
        relay(("E0", "L0"), 1)
    with jax.named_scope("attend1c"):
        attend(1, 7, 8)
    o_copy1, g_copies1 = share(1)
    with jax.named_scope("wgrad1"):
        for m in range(3):
            weight_grad(1, m)
            ring_start("E1", ("1A", "1B"), m)
            if m == 1:
                with jax.named_scope("f2_0"):
                    finish(("E0", "L0"), 1)
    with jax.named_scope("dwo1"):
        o_copy1.wait_recv()
        out_weight_grad(1)
        ring_start("L1", ("1A", "1B"))
        for m in range(3):
            ring_start("E1", ("RB", "LA"), m)
        ring_start("L1", ("RB", "LA"))

    def y_part(r, n):
        rows, cols = pl.ds(pl.multiple_of(own0 + r * HALF, HALF), HALF), pl.ds(n * HALF, HALF)
        t = dot(oo[rows, :], wo[:, cols]) + dot(o_in[rows, :], xf[pl.ds(DIM + n * HALF, HALF), pl.ds(HALF, HALF)])
        y_ref[pl.ds(r * HALF, HALF), cols] = t.astype(BF16)

    def dx_part(r, n):
        rows, cols = pl.ds(pl.multiple_of(own0 + r * HALF, HALF), HALF), pl.ds(n * HALF, HALF)
        t = None
        for m, (gr, w, w2) in enumerate(((gq, wq, xf.at[cols, pl.ds(0, HALF)]), (gk, wk, xf.at[cols, pl.ds(HALF, HALF)]),
                                         (gv, wv, xf.at[pl.ds(DIM + n * HALF, HALF), pl.ds(0, HALF)]))):
            u = dot_t(gr[rows, :], w[cols, :]) + dot_t(g_in[m, pl.ds(r * HALF, HALF), :], w2[...])
            t = u if t is None else t + u
        dx_ref[pl.ds(r * HALF, HALF), cols] = t.astype(BF16)

    for name in ("wq2", "wk2", "wv2", "wo20", "wo21"):
        loads[name].wait()
    with jax.named_scope("Y"):
        for r in range(2):
            for n in range(2):
                y_part(r, n)
    for c in g_copies0 + g_copies1:
        c.wait_recv()
    with jax.named_scope("dX0"):
        dx_part(0, 0)
    with jax.named_scope("r1E1"):
        relay(("E1", "L1"), 0)
    with jax.named_scope("dX1"):
        dx_part(0, 1)
    with jax.named_scope("f3_0"):
        finish(("E0", "L0"), 2)
    with jax.named_scope("dX2"):
        dx_part(1, 0)
    with jax.named_scope("dX3"):
        dx_part(1, 1)
    last_gens = ("E1", "L1")
    with jax.named_scope("f1_1"):
        finish(last_gens, 0)
    with jax.named_scope("sends"):
        early = sent[:-36]
        del sent[:-36]
        wait_sends(early)
    with jax.named_scope("r2_1"):
        relay(last_gens, 1)
    with jax.named_scope("f2_1"):
        finish(last_gens, 1)
    with jax.named_scope("f3_1"):
        finish(last_gens, 2)

    final = acc.at[:, :, me["z"], yat[0], me["x"]]
    last = remote("final", final, fin, partner)
    start(last)
    with jax.named_scope("sends2"):
        for g in range(2):
            for h in range(2):
                cols = pl.ds(pl.multiple_of(core * HALF + g * 256 + h * 128, 128), 128)
                dw_ref[:, cols] = acc[g, h, me["z"], yat[0], me["x"]]
        wait_sends(sent)
    with jax.named_scope("last"):
        last.wait_recv()
    for g in range(2):
        for h in range(2):
            cols = pl.ds(pl.multiple_of(other * HALF + g * 256 + h * 128, 128), 128)
            dw_ref[:, cols] = fin[g, h]
    wait_sends(sent)


def hop_shapes(part, phase):
    rest = 2 - phase
    return [pltpu.VMEM((2, 2) + (4,) * rest + (PART_ROWS[part][1], 128), F32)] * 3


def write_out(y_in, dx_in, dw_in, y_out, dx_out, dw_out, sems):
    copies = [pltpu.make_async_copy(dw_in, dw_out, sems.at[8])]
    for n in range(4):
        rows = pl.ds(n * (TOK // 4), TOK // 4)
        copies.append(pltpu.make_async_copy(y_in.at[rows], y_out.at[rows], sems.at[n]))
        copies.append(pltpu.make_async_copy(dx_in.at[rows], dx_out.at[rows], sems.at[4 + n]))
    for c in copies:
        c.start()
    for c in copies:
        c.wait()


def solution(mesh):
    act = P(("pod", "data"), "seq", None)
    scale = float((64 * SEQ) ** -0.5)

    def local(x, wq, wk, wv, wo, dy):
        vm = pltpu.VMEM
        any_ = pl.BlockSpec(memory_space=pl.ANY)
        scratch = [
            vm((SEQ, DIM), BF16), vm((DIM, SEQ), BF16), vm((SEQ, DIM), BF16),
            *[vm((DIM, HALF), BF16)] * 3, vm((HALF, DIM), BF16),
            *[vm((SEQ, GRP), F32)] * 2, *[vm((SEQ, GRP), BF16)] * 3,
            *[vm((NCH, 2, 128, 128), F32)] * 2,
            vm((SEQ, HALF), BF16), vm((SEQ, HALF), BF16), *[vm((SEQ, HALF), BF16)] * 3, vm((3, TOK, HALF), BF16),
            vm((2, 2, 4, 4, 4, ROWS, 128), F32), vm((2, 2, ROWS, 128), F32),
        ]
        for part in range(3):
            for phase in range(3):
                scratch += hop_shapes(part, phase)
        scratch += [pltpu.SemaphoreType.DMA((NUM_SEMS,)), pltpu.SemaphoreType.DMA((NUM_SEMS,)),
                    pltpu.SemaphoreType.DMA((NUM_LOCAL,))]
        held = pl.pallas_call(
            lambda *refs: kernel(scale, *refs),
            out_shape=(vm((TOK, DIM), BF16), vm((TOK, DIM), BF16), vm((ROWS, DIM), F32)),
            in_specs=[any_] * 6,
            out_specs=(pl.BlockSpec(memory_space=pltpu.VMEM),) * 3,
            scratch_shapes=scratch,
            name="layer",
            compiler_params=pltpu.CompilerParams(collective_id=0, has_side_effects=True, vmem_limit_bytes=62560000),
        )(x[0], dy[0], wq, wk, wv, wo.reshape(DIM, DIM))
        y, dx, dw = pl.pallas_call(
            write_out,
            out_shape=(jax.ShapeDtypeStruct((TOK, DIM), BF16), jax.ShapeDtypeStruct((TOK, DIM), BF16),
                       jax.ShapeDtypeStruct((ROWS, DIM), F32)),
            in_specs=[pl.BlockSpec(memory_space=pltpu.VMEM)] * 3,
            out_specs=(any_,) * 3,
            scratch_shapes=[pltpu.SemaphoreType.DMA((9,))],
            name="write_out",
            compiler_params=pltpu.CompilerParams(vmem_limit_bytes=16 * 1024 * 1024),
        )(*held)
        return y[None], dx[None], dw

    return jax.shard_map(local, mesh=mesh,
                         in_specs=(act, P(None, None), P(None, None), P(None, None), P(None, None, None), act),
                         out_specs=(act, act, P(("pod", "data"), None)), check_vma=False)
```

```python
import jax
import jax.numpy as jnp
from jax import lax
from jax.experimental import pallas as pl
from jax.experimental.pallas import tpu as pltpu
from jax.sharding import PartitionSpec as P

MESH = pl.DeviceIdType.MESH
F32 = jnp.float32
BF16 = jnp.bfloat16

TOK = 1024
SEQ = 2 * TOK
DIM = 1024
HALF = DIM // 2
GRP = 256
CHUNK = 256
NCH = SEQ // CHUNK
BLK = 512
ROWS = 64

ORDER = (("z", "y", "x"), ("y", "x", "z"), ("x", "z", "y"))
PART_ROWS = ((0, 16), (16, 24), (40, 24))
AXES = ("z", "y", "x")


def dot(a, b):
    return lax.dot_general(a, b, (((1,), (0,)), ((), ())), preferred_element_type=F32)


def dot_t(a, b):
    return lax.dot_general(a, b, (((1,), (1,)), ((), ())), preferred_element_type=F32)


def t_dot(a, b):
    return lax.dot_general(a, b, (((0,), (0,)), ((), ())), preferred_element_type=F32)


NUM_SEMS = 240
NUM_LOCAL = 14
KINDS = {"1A": (0, 2, 0, 1), "1B": (1, 2, 0, -1), "RB": (1, 1, 1, 1), "LA": (0, 3, 2, -1),
         "RA": (0, 1, 1, 1), "LB": (1, 3, 2, -1),
         "O": (slice(None), 2, 0, 2), "R": (slice(None), 1, 1, 1), "L": (slice(None), 3, 2, -1)}
RAW = ("1A", "1B", "RB", "LA")
RING = ("RB", "LA", "RA", "LB")
LAST = ("O", "R", "L")
GENS = {"E0": (0, 0, 3, None), "L0": (None, 3, 1, 0), "E1": (1, 0, 3, None), "L1": (None, 3, 1, 1)}


def when(cond, fn):
    if cond is None:
        fn()
    else:
        pl.when(cond)(fn)


def both(a, b):
    return b if a is None else a if b is None else jnp.logical_and(a, b)


def kernel(scale, x_hbm, dy_hbm, wq_hbm, wk_hbm, wv_hbm, wo_hbm,
           y_ref, dx_ref, dw_ref,
           xf, xt, dyf, wq, wk, wv, wo, sga, sgb, qg, kg, vg,
           kv_raw, qd_raw, oo, o_in, gq, gk, gv, g_in, acc, fin,
           r00, l00, m00, r01, l01, m01, r02, l02, m02,
           r10, l10, m10, r11, l11, m11, r12, l12, m12,
           r20, l20, m20, r21, l21, m21, r22, l22, m22,
           send_sem, recv_sem, local_sem):
    core = lax.axis_index("seq")
    data = lax.axis_index("data")
    me = {"z": lax.div(data, 16), "y": lax.rem(lax.div(data, 4), 4), "x": lax.rem(data, 4)}
    at = {a: [me[a]] + [lax.rem(me[a] + k, 4) for k in (1, 2, 3)] for a in AXES}
    yat = [lax.rem(v, 2) * 2 + lax.div(v, 2) for v in at["y"]]
    stride = {"z": 16, "y": 4, "x": 1}
    away = {a: [data + (at[a][k] - me[a]) * stride[a] for k in range(4)] for a in AXES}
    is_last = [v == 3 for v in at["z"]]
    not_last = [v != 3 for v in at["z"]]
    parity = [[lax.rem(v, 2) == par for v in at["y"]] for par in (0, 1)]
    conds = {}
    other = 1 - core
    hop_bufs = {(0, 0): (r00, l00, m00), (0, 1): (r01, l01, m01), (0, 2): (r02, l02, m02),
                (1, 0): (r10, l10, m10), (1, 1): (r11, l11, m11), (1, 2): (r12, l12, m12),
                (2, 0): (r20, l20, m20), (2, 1): (r21, l21, m21), (2, 2): (r22, l22, m22)}
    sem_ids = {}
    sent = []

    def device(axis, delta):
        return {"data": away[axis][delta % 4], "seq": core}

    partner = {"data": data, "seq": other}

    def remote(name, src, dst, dev):
        k = sem_ids.setdefault(name, len(sem_ids))
        assert k < NUM_SEMS
        return pltpu.make_async_remote_copy(src_ref=src, dst_ref=dst, send_sem=send_sem.at[k],
                                            recv_sem=recv_sem.at[k], device_id=dev, device_id_type=MESH)

    def start(copy):
        copy.start()
        sent.append((copy, None))

    def gen_test(gen, axis, k):
        _, m_lo, _, par = GENS[gen]
        if axis == "z":
            return ("z", m_lo != 0, k)
        if axis == "y" and par is not None:
            return ("y", par, k)
        return None

    def active(gen, part, phase, step):
        tests = [gen_test(gen, axis, 0 if p < phase else step) for p, axis in enumerate(ORDER[part][:phase + 1])]
        key = tuple(sorted(t for t in tests if t is not None))
        if key not in conds:
            cond = None
            for axis, kind, k in key:
                cond = both(cond, (is_last if kind else not_last)[k] if axis == "z" else parity[kind][k])
            conds[key] = cond
        return conds[key]

    def place(part, phase, step):
        where = {}
        for p, a in enumerate(ORDER[part][:phase + 1]):
            k = 0 if p < phase else step
            where[a] = yat[k] if a == "y" else at[a][k]
        return where

    def free_range(gen, axis, msub=None):
        _, m_lo, mn, par = GENS[gen]
        if axis == "z":
            return (m_lo, mn) if msub is None else (msub, 1)
        if axis == "y" and par is not None:
            return 2 * par, 2
        return 0, 4

    def copy_of(gen, part, phase, kind, msub=None):
        h, step, b, direction = KINDS[kind]
        g = GENS[gen][0]
        gsl = pl.ds(0, 2) if g is None else pl.ds(g, 1)
        row0, nr = PART_ROWS[part]
        where, land = place(part, phase, step), [gsl, h]
        for a in AXES:
            if a not in where:
                where[a] = pl.ds(*free_range(gen, a, msub))
                land.append(where[a])
        src = acc.at[(gsl, h, where["z"], where["y"], where["x"], pl.ds(row0, nr), slice(None))]
        return remote((gen, part, phase, kind), src, hop_bufs[part, phase][b].at[tuple(land)],
                      device(ORDER[part][phase], direction))

    def send(gen, part, phase, kind):
        cond = active(gen, part, phase, KINDS[kind][1])
        copy = copy_of(gen, part, phase, kind)
        when(cond, copy.start)
        sent.append((copy, cond))

    def ring_start(gen, kinds, m=None):
        last = m is None or m == 2
        for kind in kinds:
            for part in (1, 2, 0):
                step = KINDS[kind][1]
                cond = active(gen, part, 0, step)
                if ORDER[part][0] == "z":
                    copy = copy_of(gen, part, 0, kind)
                    when(at["z"][step] == (3 if m is None else m), copy.start)
                else:
                    copy = copy_of(gen, part, 0, kind, m)
                    when(cond, copy.start)
                if last:
                    sent.append((copy_of(gen, part, 0, kind), cond))

    def add_into(gen, part, phase, hs, step, bufs):
        row0, nr = PART_ROWS[part]
        g = GENS[gen][0]
        where, land = place(part, phase, step), []
        for a in AXES:
            if a not in where:
                where[a] = pl.ds(*free_range(gen, a))
                land.append(where[a])
        for gi in ((0, 1) if g is None else (g,)):
            for h in hs:
                spot = (gi, h, where["z"], where["y"], where["x"], pl.ds(row0, nr), slice(None))
                total = acc[spot]
                for b in bufs:
                    total = total + b[(gi, h, *land, slice(None), slice(None))]
                acc[spot] = total

    def relay(gens, phase, parts=(1, 2, 0)):
        for part in parts:
            for gen in gens:
                for got, out in (("1A", "RA"), ("1B", "LB")):
                    step = KINDS[out][1]
                    cond = active(gen, part, phase, step)
                    arrived = copy_of(gen, part, phase, got)
                    copy = copy_of(gen, part, phase, out)

                    def go():
                        arrived.wait_recv()
                        add_into(gen, part, phase, (KINDS[out][0],), step, [hop_bufs[part, phase][0]])
                        copy.start()

                    when(cond, go)
                    sent.append((copy, cond))

    def finish(gens, phase, parts=(1, 2, 0)):
        for part in parts:
            for gen in gens:
                arrivals = [copy_of(gen, part, phase, k) for k in (LAST if phase == 2 else RING)]

                def go():
                    for a in arrivals:
                        a.wait_recv()
                    add_into(gen, part, phase, (0, 1), 0, list(hop_bufs[part, phase][0 if phase == 2 else 1:]))

                when(active(gen, part, phase, 0), go)
                if phase < 2:
                    for kind in (RAW if phase == 0 else LAST):
                        send(gen, part, phase + 1, kind)

    def wait_sends(copies):
        for copy, cond in copies:
            when(cond, copy.wait_send)
        copies.clear()

    own0 = pl.multiple_of(core * TOK, TOK)
    oth0 = pl.multiple_of(other * TOK, TOK)
    barrier = pltpu.get_barrier_semaphore()
    for dev in [partner] + [device(a, s) for a in AXES for s in (1, -1)]:
        pl.semaphore_signal(barrier, inc=1, device_id=dev, device_id_type=MESH)
    own_c = pl.ds(pl.multiple_of(core * HALF, HALF), HALF)
    oth_c = pl.ds(pl.multiple_of(other * HALF, HALF), HALF)
    loads = {}

    def load(name, src, dst):
        loads[name] = pltpu.make_async_copy(src, dst, local_sem.at[len(loads)])
        loads[name].start()

    load("x0", x_hbm.at[pl.ds(0, BLK)], xf.at[pl.ds(own0, BLK)])
    for name, src, dst in (("wq", wq_hbm, wq), ("wk", wk_hbm, wk), ("wv", wv_hbm, wv)):
        load(name, src.at[:, own_c], dst)
    load("x1", x_hbm.at[pl.ds(BLK, BLK)], xf.at[pl.ds(own0 + BLK, BLK)])
    load("dy", dy_hbm, dyf.at[pl.ds(own0, TOK)])
    load("wo", wo_hbm.at[own_c], wo)

    lanes = lax.broadcasted_iota(jnp.int32, (1, 128), 1)
    first = (lanes < 64).astype(F32).astype(BF16)
    second = (lanes >= 64).astype(F32).astype(BF16)
    tri = (lax.broadcasted_iota(jnp.int32, (128, 256), 0)
           >= lax.rem(lax.broadcasted_iota(jnp.int32, (128, 256), 1), 128))

    def stacked(a, n):
        part = a[n * 128:n * 128 + 128]
        return jnp.concatenate([part * first, part * second], axis=0)

    def masked(sc):
        top = jnp.where(tri, sc[:128], 0.0).astype(BF16)
        return top if sc.shape[0] == 128 else jnp.concatenate([top, sc[128:].astype(BF16)], axis=0)

    def lower(full, extra):
        return jnp.concatenate([full[:128], full[128:] + extra], axis=0)

    def turned(s0, s1, r):
        wide = t_dot(s0, r)
        tail = jnp.concatenate([s1[:, :128].T, s1[:, 128:].T], axis=1)
        return jnp.concatenate([jnp.where(lanes < 64, wide[:128], wide[128:]), dot(tail, stacked(r, 1))], axis=0)

    block_diag = ((lax.broadcasted_iota(jnp.int32, (128, 128), 0) < 64)
                  == (lax.broadcasted_iota(jnp.int32, (128, 128), 1) < 64))

    def chunk_products(a, b, raw, base, blk):
        for n in range(blk // CHUNK):
            rs = slice(n * CHUNK, (n + 1) * CHUNK)
            p = t_dot(a[rs, :], b[rs, :])
            for j in range(2):
                cs = slice(j * 128, j * 128 + 128)
                raw[lax.div(base, CHUNK) + n, j] = p[cs, cs]

    def project_x(g, base, blk, ready=lambda name: None):
        rows = pl.ds(base, blk)
        gcols = pl.ds(g * GRP, GRP)
        xa = xf[rows, :]
        pre_act = []
        for name, w in (("wq", wq), ("wk", wk)):
            ready(name)
            pre_act.append(dot(xa, w[:, gcols]))
        ready("wv")
        v = dot(xa, wv[:, gcols]).astype(BF16)
        vg[rows, :] = v
        for a, sg, out in ((pre_act[0], sga, qg), (pre_act[1], sgb, kg)):
            s = pl.reciprocal(1.0 + jnp.exp2(a * -1.4426950408889634))
            f = a * s
            kept = f.astype(BF16)
            out[rows, :] = kept
            sg[rows, :] = s + f * (1.0 - s)
        if g == 0:
            xt[:, rows] = xa.T
        chunk_products(kept, v, kv_raw, base, blk)

    def project_dy(g, half, base):
        rows = pl.ds(base, TOK)
        do = dot_t(dyf[rows, :], wo[pl.ds(g * GRP, GRP), :]).astype(BF16)
        dx_ref[:, pl.ds(pl.multiple_of(half * GRP, GRP), GRP)] = do
        chunk_products(qg[rows, :], do, qd_raw, base, TOK)

    def scan_states():
        for raw, side, order in ((kv_raw, 0, range(NCH)), (qd_raw, 1, range(NCH - 1, -1, -1))):
            for j in range(2):
                st = jnp.zeros((128, 128), F32)
                for i in order:
                    y_ref[i * 128:i * 128 + 128, (side * 2 + j) * 128:(side * 2 + j) * 128 + 128] = st.astype(BF16)
                    st = st + jnp.where(block_diag, raw[i, j], 0.0)

    def attend(g, lo, hi):
        def body(i, _):
            rows = pl.ds(pl.multiple_of(i * CHUNK, CHUNK), CHUNK)
            srows = pl.ds(pl.multiple_of(i * 128, 128), 128)
            drows = pl.ds(pl.multiple_of(lax.rem(i, 4) * CHUNK, CHUNK), CHUNK)
            for j in range(2):
                cols = pl.ds(j * 128, 128)
                pre, suf = y_ref[srows, cols], y_ref[srows, pl.ds(256 + j * 128, 128)]
                ocols = pl.ds(g * GRP + j * 128, 128)
                q, k, v = qg[rows, cols], kg[rows, cols], vg[rows, cols]
                do = dx_ref[drows, pl.ds(pl.multiple_of(lax.div(i, 4) * GRP + j * 128, 128), 128)]
                k0, k1, v0, v1 = stacked(k, 0), stacked(k, 1), stacked(v, 0), stacked(v, 1)
                p0, p1 = masked(dot_t(q, k0)), masked(dot_t(q[128:], k1))
                d0, d1 = masked(dot_t(do, v0)), masked(dot_t(do[128:], v1))
                o = lower(dot(p0, v0) + dot(q, pre), dot(p1, v1))
                oo[rows, ocols] = (scale * o).astype(BF16)
                dq = lower(dot(d0, k0) + dot_t(do, pre), dot(d1, k1))
                gq[rows, ocols] = (scale * dq * sga[rows, cols]).astype(BF16)
                dk = dot_t(v, suf) + turned(d0, d1, q)
                gk[rows, ocols] = (scale * dk * sgb[rows, cols]).astype(BF16)
                dv = dot(k, suf) + turned(p0, p1, do)
                gv[rows, ocols] = (scale * dv).astype(BF16)
            return 0

        lax.fori_loop(lo, hi, body, 0)

    def weight_grad(g, m):
        gr = (gq, gk, gv)[m]

        for n in range(2):
            t = dot(xt[n * 512:n * 512 + 512, :], gr[:, pl.ds(g * GRP, GRP)])
            for h in range(2):
                for yy in range(2):
                    for xx in range(4):
                        r = yy * 256 + xx * 64
                        acc[g, h, m, yy * 2 + n, xx] = t[r:r + 64, h * 128:h * 128 + 128]

    def out_weight_grad(g):
        rhs_cols = pl.ds(pl.multiple_of(core * HALF, HALF), HALF)
        for src, who in ((oo, core), (o_in, other)):
            t = t_dot(src[:, pl.ds(g * GRP, GRP)], dyf[:, rhs_cols])
            for gg in range(2):
                for h in range(2):
                    for xx in range(4):
                        c0 = gg * 256 + h * 128
                        acc[gg, h, 3, g * 2 + who, xx] = t[xx * 64:xx * 64 + 64, c0:c0 + 128]

    def share(g):
        cols = pl.ds(g * GRP, GRP)
        o_copy = remote(("o", g), oo.at[:, cols], o_in.at[:, cols], partner)
        start(o_copy)
        g_copies = []
        for m, gr in enumerate((gq, gk, gv)):
            g_copies.append(remote(("g", g, m), gr.at[pl.ds(oth0, TOK), cols], g_in.at[m, :, cols], partner))
            start(g_copies[-1])
        return o_copy, g_copies

    a0 = core * TOK
    with jax.named_scope("barrier"):
        pl.semaphore_wait(barrier, 7)
    x_send = remote("x", x_hbm, xf.at[pl.ds(own0, TOK)], partner)
    dy_send = remote("dy", dy_hbm, dyf.at[pl.ds(own0, TOK)], partner)
    start(x_send)
    start(dy_send)
    with jax.named_scope("load0"):
        loads["x0"].wait()
    project_x(0, pl.multiple_of(a0, BLK), BLK, lambda name: loads[name].wait())
    with jax.named_scope("projA0"):
        loads["x1"].wait()
        project_x(0, pl.multiple_of(a0 + BLK, BLK), BLK)
        for name in ("dy", "wo"):
            loads[name].wait()
        project_dy(0, core, own0)
    with jax.named_scope("xrecv"):
        x_send.wait_recv()
    with jax.named_scope("projB0"):
        for n in range(2):
            project_x(0, pl.multiple_of(oth0 + n * BLK, BLK), BLK)
    with jax.named_scope("dyrecv"):
        dy_send.wait_recv()
    with jax.named_scope("projBd0"):
        project_dy(0, other, oth0)
    with jax.named_scope("scan0"):
        scan_states()
    with jax.named_scope("attend0"):
        attend(0, 0, NCH)
    o_copy0, g_copies0 = share(0)
    with jax.named_scope("wgrad0"):
        for m in range(3):
            weight_grad(0, m)
            ring_start("E0", ("1A", "1B"), m)
    with jax.named_scope("dwo0"):
        o_copy0.wait_recv()
        out_weight_grad(0)
        ring_start("L0", ("1A", "1B"))
        for m in range(3):
            ring_start("E0", ("RB", "LA"), m)
        ring_start("L0", ("RB", "LA"))

    with jax.named_scope("projA1"):
        for n in range(2):
            project_x(1, pl.multiple_of(own0 + n * BLK, BLK), BLK)
        project_dy(1, core, own0)
    with jax.named_scope("r1E0"):
        relay(("E0",), 0)
    with jax.named_scope("projB1a"):
        for n in range(2):
            project_x(1, pl.multiple_of(oth0 + n * BLK, BLK), BLK)
    with jax.named_scope("r1L0"):
        relay(("L0",), 0)
    with jax.named_scope("projB1b"):
        project_dy(1, other, oth0)
    load("wq2", wq_hbm.at[:, oth_c], xf.at[pl.ds(0, DIM), pl.ds(0, HALF)])
    load("wk2", wk_hbm.at[:, oth_c], xf.at[pl.ds(0, DIM), pl.ds(HALF, HALF)])
    load("wv2", wv_hbm.at[:, oth_c], xf.at[pl.ds(DIM, DIM), pl.ds(0, HALF)])
    for n in range(2):
        load(f"wo2{n}", wo_hbm.at[oth_c, pl.ds(n * HALF, HALF)], xf.at[pl.ds(DIM + n * HALF, HALF), pl.ds(HALF, HALF)])
    with jax.named_scope("scan1"):
        scan_states()
    with jax.named_scope("attend1a"):
        attend(1, 0, 4)
    with jax.named_scope("f1_0"):
        finish(("E0", "L0"), 0)
    with jax.named_scope("attend1b"):
        attend(1, 4, 8)
    o_copy1, g_copies1 = share(1)
    with jax.named_scope("r2_0"):
        relay(("E0", "L0"), 1)
    with jax.named_scope("wgrad1"):
        for m in range(3):
            weight_grad(1, m)
            ring_start("E1", ("1A", "1B"), m)
    with jax.named_scope("dwo1"):
        o_copy1.wait_recv()
        out_weight_grad(1)
        ring_start("L1", ("1A", "1B"))
        for m in range(3):
            ring_start("E1", ("RB", "LA"), m)
        ring_start("L1", ("RB", "LA"))
    with jax.named_scope("f2_0"):
        finish(("E0", "L0"), 1)

    def y_part(r, n):
        rows, cols = pl.ds(pl.multiple_of(own0 + r * HALF, HALF), HALF), pl.ds(n * HALF, HALF)
        t = dot(oo[rows, :], wo[:, cols]) + dot(o_in[rows, :], xf[pl.ds(DIM + n * HALF, HALF), pl.ds(HALF, HALF)])
        y_ref[pl.ds(r * HALF, HALF), cols] = t.astype(BF16)

    def dx_part(r, n):
        rows, cols = pl.ds(pl.multiple_of(own0 + r * HALF, HALF), HALF), pl.ds(n * HALF, HALF)
        t = None
        for m, (gr, w, w2) in enumerate(((gq, wq, xf.at[cols, pl.ds(0, HALF)]), (gk, wk, xf.at[cols, pl.ds(HALF, HALF)]),
                                         (gv, wv, xf.at[pl.ds(DIM + n * HALF, HALF), pl.ds(0, HALF)]))):
            u = dot_t(gr[rows, :], w[cols, :]) + dot_t(g_in[m, pl.ds(r * HALF, HALF), :], w2[...])
            t = u if t is None else t + u
        dx_ref[pl.ds(r * HALF, HALF), cols] = t.astype(BF16)

    for name in ("wq2", "wk2", "wv2", "wo20", "wo21"):
        loads[name].wait()
    with jax.named_scope("Y"):
        for r in range(2):
            for n in range(2):
                y_part(r, n)
    for c in g_copies0 + g_copies1:
        c.wait_recv()
    with jax.named_scope("dX0"):
        dx_part(0, 0)
    with jax.named_scope("r1E1"):
        relay(("E1", "L1"), 0)
    with jax.named_scope("dX1"):
        dx_part(0, 1)
    with jax.named_scope("dX2"):
        dx_part(1, 0)
    with jax.named_scope("f3_0"):
        finish(("E0", "L0"), 2)
    with jax.named_scope("dX3"):
        dx_part(1, 1)
    last_gens = ("E1", "L1")
    with jax.named_scope("f1_1"):
        finish(last_gens, 0)
    with jax.named_scope("sends"):
        early = sent[:-36]
        del sent[:-36]
        wait_sends(early)
    with jax.named_scope("r2_1"):
        relay(last_gens, 1)
    with jax.named_scope("f2_1"):
        finish(last_gens, 1)
    with jax.named_scope("f3_1"):
        finish(last_gens, 2)

    final = acc.at[:, :, me["z"], yat[0], me["x"]]
    last = remote("final", final, fin, partner)
    start(last)
    with jax.named_scope("sends2"):
        for g in range(2):
            for h in range(2):
                cols = pl.ds(pl.multiple_of(core * HALF + g * 256 + h * 128, 128), 128)
                dw_ref[:, cols] = acc[g, h, me["z"], yat[0], me["x"]]
        wait_sends(sent)
    with jax.named_scope("last"):
        last.wait_recv()
    for g in range(2):
        for h in range(2):
            cols = pl.ds(pl.multiple_of(other * HALF + g * 256 + h * 128, 128), 128)
            dw_ref[:, cols] = fin[g, h]
    wait_sends(sent)


def hop_shapes(part, phase):
    rest = 2 - phase
    return [pltpu.VMEM((2, 2) + (4,) * rest + (PART_ROWS[part][1], 128), F32)] * 3


def write_out(y_in, dx_in, dw_in, y_out, dx_out, dw_out, sems):
    copies = [pltpu.make_async_copy(dw_in, dw_out, sems.at[8])]
    for n in range(4):
        rows = pl.ds(n * (TOK // 4), TOK // 4)
        copies.append(pltpu.make_async_copy(y_in.at[rows], y_out.at[rows], sems.at[n]))
        copies.append(pltpu.make_async_copy(dx_in.at[rows], dx_out.at[rows], sems.at[4 + n]))
    for c in copies:
        c.start()
    for c in copies:
        c.wait()


def solution(mesh):
    act = P(("pod", "data"), "seq", None)
    scale = float((64 * SEQ) ** -0.5)

    def local(x, wq, wk, wv, wo, dy):
        vm = pltpu.VMEM
        any_ = pl.BlockSpec(memory_space=pl.ANY)
        scratch = [
            vm((SEQ, DIM), BF16), vm((DIM, SEQ), BF16), vm((SEQ, DIM), BF16),
            *[vm((DIM, HALF), BF16)] * 3, vm((HALF, DIM), BF16),
            *[vm((SEQ, GRP), F32)] * 2, *[vm((SEQ, GRP), BF16)] * 3,
            *[vm((NCH, 2, 128, 128), F32)] * 2,
            vm((SEQ, HALF), BF16), vm((SEQ, HALF), BF16), *[vm((SEQ, HALF), BF16)] * 3, vm((3, TOK, HALF), BF16),
            vm((2, 2, 4, 4, 4, ROWS, 128), F32), vm((2, 2, ROWS, 128), F32),
        ]
        for part in range(3):
            for phase in range(3):
                scratch += hop_shapes(part, phase)
        scratch += [pltpu.SemaphoreType.DMA((NUM_SEMS,)), pltpu.SemaphoreType.DMA((NUM_SEMS,)),
                    pltpu.SemaphoreType.DMA((NUM_LOCAL,))]
        held = pl.pallas_call(
            lambda *refs: kernel(scale, *refs),
            out_shape=(vm((TOK, DIM), BF16), vm((TOK, DIM), BF16), vm((ROWS, DIM), F32)),
            in_specs=[any_] * 6,
            out_specs=(pl.BlockSpec(memory_space=pltpu.VMEM),) * 3,
            scratch_shapes=scratch,
            name="layer",
            compiler_params=pltpu.CompilerParams(collective_id=0, has_side_effects=True, vmem_limit_bytes=62560000),
        )(x[0], dy[0], wq, wk, wv, wo.reshape(DIM, DIM))
        y, dx, dw = pl.pallas_call(
            write_out,
            out_shape=(jax.ShapeDtypeStruct((TOK, DIM), BF16), jax.ShapeDtypeStruct((TOK, DIM), BF16),
                       jax.ShapeDtypeStruct((ROWS, DIM), F32)),
            in_specs=[pl.BlockSpec(memory_space=pltpu.VMEM)] * 3,
            out_specs=(any_,) * 3,
            scratch_shapes=[pltpu.SemaphoreType.DMA((9,))],
            name="write_out",
            compiler_params=pltpu.CompilerParams(vmem_limit_bytes=16 * 1024 * 1024),
        )(*held)
        return y[None], dx[None], dw

    return jax.shard_map(local, mesh=mesh,
                         in_specs=(act, P(None, None), P(None, None), P(None, None), P(None, None, None), act),
                         out_specs=(act, act, P(("pod", "data"), None)), check_vma=False)
```

```python
import jax
import jax.numpy as jnp
from jax import lax
from jax.experimental import pallas as pl
from jax.experimental.pallas import tpu as pltpu
from jax.sharding import PartitionSpec as P

MESH = pl.DeviceIdType.MESH
F32 = jnp.float32
BF16 = jnp.bfloat16

TOK = 1024
SEQ = 2 * TOK
DIM = 1024
HALF = DIM // 2
GRP = 256
CHUNK = 256
NCH = SEQ // CHUNK
BLK = 512
ROWS = 64

ORDER = (("z", "y", "x"), ("y", "x", "z"), ("x", "z", "y"))
PART_ROWS = ((0, 16), (16, 24), (40, 24))
AXES = ("z", "y", "x")


def dot(a, b):
    return lax.dot_general(a, b, (((1,), (0,)), ((), ())), preferred_element_type=F32)


def dot_t(a, b):
    return lax.dot_general(a, b, (((1,), (1,)), ((), ())), preferred_element_type=F32)


def t_dot(a, b):
    return lax.dot_general(a, b, (((0,), (0,)), ((), ())), preferred_element_type=F32)


NUM_SEMS = 240
NUM_LOCAL = 14
KINDS = {"1A": (0, 2, 0, 1), "1B": (1, 2, 0, -1), "RB": (1, 1, 1, 1), "LA": (0, 3, 2, -1),
         "RA": (0, 1, 1, 1), "LB": (1, 3, 2, -1),
         "O": (slice(None), 2, 0, 2), "R": (slice(None), 1, 1, 1), "L": (slice(None), 3, 2, -1)}
RAW = ("1A", "1B", "RB", "LA")
RING = ("RB", "LA", "RA", "LB")
LAST = ("O", "R", "L")
GENS = {"E0": (0, 0, 3, None), "L0": (None, 3, 1, 0), "E1": (1, 0, 3, None), "L1": (None, 3, 1, 1)}


def when(cond, fn):
    if cond is None:
        fn()
    else:
        pl.when(cond)(fn)


def both(a, b):
    return b if a is None else a if b is None else jnp.logical_and(a, b)


def kernel(scale, x_hbm, dy_hbm, wq_hbm, wk_hbm, wv_hbm, wo_hbm,
           y_ref, dx_ref, dw_ref,
           xf, xt, dyf, wq, wk, wv, wo, sga, sgb, qg, kg, vg,
           kv_raw, qd_raw, oo, o_in, gq, gk, gv, g_in, acc, fin,
           r00, l00, m00, r01, l01, m01, r02, l02, m02,
           r10, l10, m10, r11, l11, m11, r12, l12, m12,
           r20, l20, m20, r21, l21, m21, r22, l22, m22,
           send_sem, recv_sem, local_sem):
    core = lax.axis_index("seq")
    data = lax.axis_index("data")
    me = {"z": lax.div(data, 16), "y": lax.rem(lax.div(data, 4), 4), "x": lax.rem(data, 4)}
    at = {a: [me[a]] + [lax.rem(me[a] + k, 4) for k in (1, 2, 3)] for a in AXES}
    yat = [lax.rem(v, 2) * 2 + lax.div(v, 2) for v in at["y"]]
    stride = {"z": 16, "y": 4, "x": 1}
    away = {a: [data + (at[a][k] - me[a]) * stride[a] for k in range(4)] for a in AXES}
    is_last = [v == 3 for v in at["z"]]
    not_last = [v != 3 for v in at["z"]]
    parity = [[lax.rem(v, 2) == par for v in at["y"]] for par in (0, 1)]
    conds = {}
    other = 1 - core
    hop_bufs = {(0, 0): (r00, l00, m00), (0, 1): (r01, l01, m01), (0, 2): (r02, l02, m02),
                (1, 0): (r10, l10, m10), (1, 1): (r11, l11, m11), (1, 2): (r12, l12, m12),
                (2, 0): (r20, l20, m20), (2, 1): (r21, l21, m21), (2, 2): (r22, l22, m22)}
    sem_ids = {}
    sent = []

    def device(axis, delta):
        return {"data": away[axis][delta % 4], "seq": core}

    partner = {"data": data, "seq": other}

    def remote(name, src, dst, dev):
        k = sem_ids.setdefault(name, len(sem_ids))
        assert k < NUM_SEMS
        return pltpu.make_async_remote_copy(src_ref=src, dst_ref=dst, send_sem=send_sem.at[k],
                                            recv_sem=recv_sem.at[k], device_id=dev, device_id_type=MESH)

    def start(copy):
        copy.start()
        sent.append((copy, None))

    def gen_test(gen, axis, k):
        _, m_lo, _, par = GENS[gen]
        if axis == "z":
            return ("z", m_lo != 0, k)
        if axis == "y" and par is not None:
            return ("y", par, k)
        return None

    def active(gen, part, phase, step):
        tests = [gen_test(gen, axis, 0 if p < phase else step) for p, axis in enumerate(ORDER[part][:phase + 1])]
        key = tuple(sorted(t for t in tests if t is not None))
        if key not in conds:
            cond = None
            for axis, kind, k in key:
                cond = both(cond, (is_last if kind else not_last)[k] if axis == "z" else parity[kind][k])
            conds[key] = cond
        return conds[key]

    def place(part, phase, step):
        where = {}
        for p, a in enumerate(ORDER[part][:phase + 1]):
            k = 0 if p < phase else step
            where[a] = yat[k] if a == "y" else at[a][k]
        return where

    def free_range(gen, axis, msub=None):
        _, m_lo, mn, par = GENS[gen]
        if axis == "z":
            return (m_lo, mn) if msub is None else (msub, 1)
        if axis == "y" and par is not None:
            return 2 * par, 2
        return 0, 4

    def copy_of(gen, part, phase, kind, msub=None):
        h, step, b, direction = KINDS[kind]
        g = GENS[gen][0]
        gsl = pl.ds(0, 2) if g is None else pl.ds(g, 1)
        row0, nr = PART_ROWS[part]
        where, land = place(part, phase, step), [gsl, h]
        for a in AXES:
            if a not in where:
                where[a] = pl.ds(*free_range(gen, a, msub))
                land.append(where[a])
        src = acc.at[(gsl, h, where["z"], where["y"], where["x"], pl.ds(row0, nr), slice(None))]
        return remote((gen, part, phase, kind), src, hop_bufs[part, phase][b].at[tuple(land)],
                      device(ORDER[part][phase], direction))

    def send(gen, part, phase, kind):
        cond = active(gen, part, phase, KINDS[kind][1])
        copy = copy_of(gen, part, phase, kind)
        when(cond, copy.start)
        sent.append((copy, cond))

    def ring_start(gen, kinds, m=None):
        last = m is None or m == 2
        for kind in kinds:
            for part in (1, 2, 0):
                step = KINDS[kind][1]
                cond = active(gen, part, 0, step)
                if ORDER[part][0] == "z":
                    copy = copy_of(gen, part, 0, kind)
                    when(at["z"][step] == (3 if m is None else m), copy.start)
                else:
                    copy = copy_of(gen, part, 0, kind, m)
                    when(cond, copy.start)
                if last:
                    sent.append((copy_of(gen, part, 0, kind), cond))

    def add_into(gen, part, phase, hs, step, bufs):
        row0, nr = PART_ROWS[part]
        g = GENS[gen][0]
        where, land = place(part, phase, step), []
        for a in AXES:
            if a not in where:
                where[a] = pl.ds(*free_range(gen, a))
                land.append(where[a])
        for gi in ((0, 1) if g is None else (g,)):
            for h in hs:
                spot = (gi, h, where["z"], where["y"], where["x"], pl.ds(row0, nr), slice(None))
                total = acc[spot]
                for b in bufs:
                    total = total + b[(gi, h, *land, slice(None), slice(None))]
                acc[spot] = total

    def relay(gens, phase, parts=(1, 2, 0)):
        for part in parts:
            for gen in gens:
                for got, out in (("1A", "RA"), ("1B", "LB")):
                    step = KINDS[out][1]
                    cond = active(gen, part, phase, step)
                    arrived = copy_of(gen, part, phase, got)
                    copy = copy_of(gen, part, phase, out)

                    def go():
                        arrived.wait_recv()
                        add_into(gen, part, phase, (KINDS[out][0],), step, [hop_bufs[part, phase][0]])
                        copy.start()

                    when(cond, go)
                    sent.append((copy, cond))

    def finish(gens, phase, parts=(1, 2, 0)):
        for part in parts:
            for gen in gens:
                arrivals = [copy_of(gen, part, phase, k) for k in (LAST if phase == 2 else RING)]

                def go():
                    for a in arrivals:
                        a.wait_recv()
                    add_into(gen, part, phase, (0, 1), 0, list(hop_bufs[part, phase][0 if phase == 2 else 1:]))

                when(active(gen, part, phase, 0), go)
                if phase < 2:
                    for kind in (RAW if phase == 0 else LAST):
                        send(gen, part, phase + 1, kind)

    def wait_sends(copies):
        for copy, cond in copies:
            when(cond, copy.wait_send)
        copies.clear()

    own0 = pl.multiple_of(core * TOK, TOK)
    oth0 = pl.multiple_of(other * TOK, TOK)
    barrier = pltpu.get_barrier_semaphore()
    for dev in [partner] + [device(a, s) for a in AXES for s in (1, -1)]:
        pl.semaphore_signal(barrier, inc=1, device_id=dev, device_id_type=MESH)
    own_c = pl.ds(pl.multiple_of(core * HALF, HALF), HALF)
    oth_c = pl.ds(pl.multiple_of(other * HALF, HALF), HALF)
    loads = {}

    def load(name, src, dst):
        loads[name] = pltpu.make_async_copy(src, dst, local_sem.at[len(loads)])
        loads[name].start()

    load("x0", x_hbm.at[pl.ds(0, BLK)], xf.at[pl.ds(own0, BLK)])
    for name, src, dst in (("wq", wq_hbm, wq), ("wk", wk_hbm, wk), ("wv", wv_hbm, wv)):
        load(name, src.at[:, own_c], dst)
    load("x1", x_hbm.at[pl.ds(BLK, BLK)], xf.at[pl.ds(own0 + BLK, BLK)])
    load("dy", dy_hbm, dyf.at[pl.ds(own0, TOK)])
    load("wo", wo_hbm.at[own_c], wo)

    lanes = lax.broadcasted_iota(jnp.int32, (1, 128), 1)
    first = (lanes < 64).astype(F32).astype(BF16)
    second = (lanes >= 64).astype(F32).astype(BF16)
    tri = (lax.broadcasted_iota(jnp.int32, (128, 256), 0)
           >= lax.rem(lax.broadcasted_iota(jnp.int32, (128, 256), 1), 128))

    def stacked(a, n):
        part = a[n * 128:n * 128 + 128]
        return jnp.concatenate([part * first, part * second], axis=0)

    def masked(sc):
        top = jnp.where(tri, sc[:128], 0.0).astype(BF16)
        return top if sc.shape[0] == 128 else jnp.concatenate([top, sc[128:].astype(BF16)], axis=0)

    def lower(full, extra):
        return jnp.concatenate([full[:128], full[128:] + extra], axis=0)

    def turned(s0, s1, r):
        wide = t_dot(s0, r)
        tail = jnp.concatenate([s1[:, :128].T, s1[:, 128:].T], axis=1)
        return jnp.concatenate([jnp.where(lanes < 64, wide[:128], wide[128:]), dot(tail, stacked(r, 1))], axis=0)

    block_diag = ((lax.broadcasted_iota(jnp.int32, (128, 128), 0) < 64)
                  == (lax.broadcasted_iota(jnp.int32, (128, 128), 1) < 64))

    def chunk_products(a, b, raw, base, blk):
        for n in range(blk // CHUNK):
            rs = slice(n * CHUNK, (n + 1) * CHUNK)
            p = t_dot(a[rs, :], b[rs, :])
            for j in range(2):
                cs = slice(j * 128, j * 128 + 128)
                raw[lax.div(base, CHUNK) + n, j] = p[cs, cs]

    def project_x(g, base, blk, ready=lambda name: None):
        rows = pl.ds(base, blk)
        gcols = pl.ds(g * GRP, GRP)
        xa = xf[rows, :]
        pre_act = []
        for name, w in (("wq", wq), ("wk", wk)):
            ready(name)
            pre_act.append(dot(xa, w[:, gcols]))
        ready("wv")
        v = dot(xa, wv[:, gcols]).astype(BF16)
        vg[rows, :] = v
        for a, sg, out in ((pre_act[0], sga, qg), (pre_act[1], sgb, kg)):
            s = pl.reciprocal(1.0 + jnp.exp2(a * -1.4426950408889634))
            f = a * s
            kept = f.astype(BF16)
            out[rows, :] = kept
            sg[rows, :] = s + f * (1.0 - s)
        if g == 0:
            xt[:, rows] = xa.T
        chunk_products(kept, v, kv_raw, base, blk)

    def project_dy(g, half, base):
        rows = pl.ds(base, TOK)
        do = dot_t(dyf[rows, :], wo[pl.ds(g * GRP, GRP), :]).astype(BF16)
        dx_ref[:, pl.ds(pl.multiple_of(half * GRP, GRP), GRP)] = do
        chunk_products(qg[rows, :], do, qd_raw, base, TOK)

    def scan_states():
        for raw, side, order in ((kv_raw, 0, range(NCH)), (qd_raw, 1, range(NCH - 1, -1, -1))):
            for j in range(2):
                st = jnp.zeros((128, 128), F32)
                for i in order:
                    y_ref[i * 128:i * 128 + 128, (side * 2 + j) * 128:(side * 2 + j) * 128 + 128] = st.astype(BF16)
                    st = st + jnp.where(block_diag, raw[i, j], 0.0)

    def attend(g, lo, hi):
        def body(i, _):
            rows = pl.ds(pl.multiple_of(i * CHUNK, CHUNK), CHUNK)
            srows = pl.ds(pl.multiple_of(i * 128, 128), 128)
            drows = pl.ds(pl.multiple_of(lax.rem(i, 4) * CHUNK, CHUNK), CHUNK)
            for j in range(2):
                cols = pl.ds(j * 128, 128)
                pre, suf = y_ref[srows, cols], y_ref[srows, pl.ds(256 + j * 128, 128)]
                ocols = pl.ds(g * GRP + j * 128, 128)
                q, k, v = qg[rows, cols], kg[rows, cols], vg[rows, cols]
                do = dx_ref[drows, pl.ds(pl.multiple_of(lax.div(i, 4) * GRP + j * 128, 128), 128)]
                k0, k1, v0, v1 = stacked(k, 0), stacked(k, 1), stacked(v, 0), stacked(v, 1)
                p0, p1 = masked(dot_t(q, k0)), masked(dot_t(q[128:], k1))
                d0, d1 = masked(dot_t(do, v0)), masked(dot_t(do[128:], v1))
                o = lower(dot(p0, v0) + dot(q, pre), dot(p1, v1))
                oo[rows, ocols] = (scale * o).astype(BF16)
                dq = lower(dot(d0, k0) + dot_t(do, pre), dot(d1, k1))
                gq[rows, ocols] = (scale * dq * sga[rows, cols]).astype(BF16)
                dk = dot_t(v, suf) + turned(d0, d1, q)
                gk[rows, ocols] = (scale * dk * sgb[rows, cols]).astype(BF16)
                dv = dot(k, suf) + turned(p0, p1, do)
                gv[rows, ocols] = (scale * dv).astype(BF16)
            return 0

        lax.fori_loop(lo, hi, body, 0, unroll=2)

    def weight_grad(g, m):
        gr = (gq, gk, gv)[m]

        for n in range(2):
            t = dot(xt[n * 512:n * 512 + 512, :], gr[:, pl.ds(g * GRP, GRP)])
            for h in range(2):
                for yy in range(2):
                    for xx in range(4):
                        r = yy * 256 + xx * 64
                        acc[g, h, m, yy * 2 + n, xx] = t[r:r + 64, h * 128:h * 128 + 128]

    def out_weight_grad(g):
        rhs_cols = pl.ds(pl.multiple_of(core * HALF, HALF), HALF)
        for src, who in ((oo, core), (o_in, other)):
            t = t_dot(src[:, pl.ds(g * GRP, GRP)], dyf[:, rhs_cols])
            for gg in range(2):
                for h in range(2):
                    for xx in range(4):
                        c0 = gg * 256 + h * 128
                        acc[gg, h, 3, g * 2 + who, xx] = t[xx * 64:xx * 64 + 64, c0:c0 + 128]

    def share(g):
        cols = pl.ds(g * GRP, GRP)
        o_copy = remote(("o", g), oo.at[:, cols], o_in.at[:, cols], partner)
        start(o_copy)
        g_copies = []
        for m, gr in enumerate((gq, gk, gv)):
            g_copies.append(remote(("g", g, m), gr.at[pl.ds(oth0, TOK), cols], g_in.at[m, :, cols], partner))
            start(g_copies[-1])
        return o_copy, g_copies

    a0 = core * TOK
    with jax.named_scope("barrier"):
        pl.semaphore_wait(barrier, 7)
    x_send = remote("x", x_hbm, xf.at[pl.ds(own0, TOK)], partner)
    dy_send = remote("dy", dy_hbm, dyf.at[pl.ds(own0, TOK)], partner)
    start(x_send)
    start(dy_send)
    with jax.named_scope("load0"):
        loads["x0"].wait()
    project_x(0, pl.multiple_of(a0, BLK), BLK, lambda name: loads[name].wait())
    with jax.named_scope("projA0"):
        loads["x1"].wait()
        project_x(0, pl.multiple_of(a0 + BLK, BLK), BLK)
        for name in ("dy", "wo"):
            loads[name].wait()
        project_dy(0, core, own0)
    with jax.named_scope("xrecv"):
        x_send.wait_recv()
    with jax.named_scope("projB0"):
        for n in range(2):
            project_x(0, pl.multiple_of(oth0 + n * BLK, BLK), BLK)
    with jax.named_scope("dyrecv"):
        dy_send.wait_recv()
    with jax.named_scope("projBd0"):
        project_dy(0, other, oth0)
    with jax.named_scope("scan0"):
        scan_states()
    with jax.named_scope("attend0"):
        attend(0, 0, NCH)
    o_copy0, g_copies0 = share(0)
    with jax.named_scope("wgrad0"):
        for m in range(3):
            weight_grad(0, m)
            ring_start("E0", ("1A", "1B"), m)
    with jax.named_scope("dwo0"):
        o_copy0.wait_recv()
        out_weight_grad(0)
        ring_start("L0", ("1A", "1B"))
        for m in range(3):
            ring_start("E0", ("RB", "LA"), m)
        ring_start("L0", ("RB", "LA"))

    with jax.named_scope("projA1"):
        for n in range(2):
            project_x(1, pl.multiple_of(own0 + n * BLK, BLK), BLK)
        project_dy(1, core, own0)
    with jax.named_scope("r1E0"):
        relay(("E0",), 0)
    with jax.named_scope("projB1"):
        for n in range(2):
            project_x(1, pl.multiple_of(oth0 + n * BLK, BLK), BLK)
        project_dy(1, other, oth0)
    with jax.named_scope("r1L0"):
        relay(("L0",), 0)
    load("wq2", wq_hbm.at[:, oth_c], xf.at[pl.ds(0, DIM), pl.ds(0, HALF)])
    load("wk2", wk_hbm.at[:, oth_c], xf.at[pl.ds(0, DIM), pl.ds(HALF, HALF)])
    load("wv2", wv_hbm.at[:, oth_c], xf.at[pl.ds(DIM, DIM), pl.ds(0, HALF)])
    for n in range(2):
        load(f"wo2{n}", wo_hbm.at[oth_c, pl.ds(n * HALF, HALF)], xf.at[pl.ds(DIM + n * HALF, HALF), pl.ds(HALF, HALF)])
    with jax.named_scope("scan1"):
        scan_states()
    with jax.named_scope("attend1a"):
        attend(1, 0, 4)
    with jax.named_scope("f1_0"):
        finish(("E0", "L0"), 0)
    with jax.named_scope("attend1b"):
        attend(1, 4, 8)
    o_copy1, g_copies1 = share(1)
    with jax.named_scope("r2_0"):
        relay(("E0", "L0"), 1)
    with jax.named_scope("wgrad1"):
        for m in range(3):
            weight_grad(1, m)
            ring_start("E1", ("1A", "1B"), m)
            if m:
                ring_start("E1", ("RB", "LA"), m - 1)
    with jax.named_scope("dwo1"):
        o_copy1.wait_recv()
        out_weight_grad(1)
        ring_start("L1", ("1A", "1B"))
        ring_start("E1", ("RB", "LA"), 2)
        ring_start("L1", ("RB", "LA"))
    with jax.named_scope("f2_0"):
        finish(("E0", "L0"), 1)

    def y_part(r, n):
        rows, cols = pl.ds(pl.multiple_of(own0 + r * HALF, HALF), HALF), pl.ds(n * HALF, HALF)
        t = dot(oo[rows, :], wo[:, cols]) + dot(o_in[rows, :], xf[pl.ds(DIM + n * HALF, HALF), pl.ds(HALF, HALF)])
        y_ref[pl.ds(r * HALF, HALF), cols] = t.astype(BF16)

    def dx_part(r, n):
        rows, cols = pl.ds(pl.multiple_of(own0 + r * HALF, HALF), HALF), pl.ds(n * HALF, HALF)
        t = None
        for m, (gr, w, w2) in enumerate(((gq, wq, xf.at[cols, pl.ds(0, HALF)]), (gk, wk, xf.at[cols, pl.ds(HALF, HALF)]),
                                         (gv, wv, xf.at[pl.ds(DIM + n * HALF, HALF), pl.ds(0, HALF)]))):
            u = dot_t(gr[rows, :], w[cols, :]) + dot_t(g_in[m, pl.ds(r * HALF, HALF), :], w2[...])
            t = u if t is None else t + u
        dx_ref[pl.ds(r * HALF, HALF), cols] = t.astype(BF16)

    for name in ("wq2", "wk2", "wv2", "wo20", "wo21"):
        loads[name].wait()
    with jax.named_scope("Y"):
        for r in range(2):
            for n in range(2):
                y_part(r, n)
    for c in g_copies0 + g_copies1:
        c.wait_recv()
    with jax.named_scope("dX0"):
        dx_part(0, 0)
    with jax.named_scope("r1E1"):
        relay(("E1", "L1"), 0)
    with jax.named_scope("dX1"):
        dx_part(0, 1)
    with jax.named_scope("dX2"):
        dx_part(1, 0)
    with jax.named_scope("f3_0"):
        finish(("E0", "L0"), 2)
    with jax.named_scope("dX3"):
        dx_part(1, 1)
    last_gens = ("E1", "L1")
    with jax.named_scope("f1_1"):
        finish(last_gens, 0)
    with jax.named_scope("sends"):
        early = sent[:-36]
        del sent[:-36]
        wait_sends(early)
    with jax.named_scope("r2_1"):
        relay(last_gens, 1)
    with jax.named_scope("f2_1"):
        finish(last_gens, 1)
    with jax.named_scope("f3_1"):
        finish(last_gens, 2)

    final = acc.at[:, :, me["z"], yat[0], me["x"]]
    last = remote("final", final, fin, partner)
    start(last)
    with jax.named_scope("sends2"):
        for g in range(2):
            for h in range(2):
                cols = pl.ds(pl.multiple_of(core * HALF + g * 256 + h * 128, 128), 128)
                dw_ref[:, cols] = acc[g, h, me["z"], yat[0], me["x"]]
        wait_sends(sent)
    with jax.named_scope("last"):
        last.wait_recv()
    for g in range(2):
        for h in range(2):
            cols = pl.ds(pl.multiple_of(other * HALF + g * 256 + h * 128, 128), 128)
            dw_ref[:, cols] = fin[g, h]
    wait_sends(sent)


def hop_shapes(part, phase):
    rest = 2 - phase
    return [pltpu.VMEM((2, 2) + (4,) * rest + (PART_ROWS[part][1], 128), F32)] * 3


def write_out(y_in, dx_in, dw_in, y_out, dx_out, dw_out, sems):
    copies = [pltpu.make_async_copy(dw_in, dw_out, sems.at[8])]
    for n in range(4):
        rows = pl.ds(n * (TOK // 4), TOK // 4)
        copies.append(pltpu.make_async_copy(y_in.at[rows], y_out.at[rows], sems.at[n]))
        copies.append(pltpu.make_async_copy(dx_in.at[rows], dx_out.at[rows], sems.at[4 + n]))
    for c in copies:
        c.start()
    for c in copies:
        c.wait()


def solution(mesh):
    act = P(("pod", "data"), "seq", None)
    scale = float((64 * SEQ) ** -0.5)

    def local(x, wq, wk, wv, wo, dy):
        vm = pltpu.VMEM
        any_ = pl.BlockSpec(memory_space=pl.ANY)
        scratch = [
            vm((SEQ, DIM), BF16), vm((DIM, SEQ), BF16), vm((SEQ, DIM), BF16),
            *[vm((DIM, HALF), BF16)] * 3, vm((HALF, DIM), BF16),
            *[vm((SEQ, GRP), F32)] * 2, *[vm((SEQ, GRP), BF16)] * 3,
            *[vm((NCH, 2, 128, 128), F32)] * 2,
            vm((SEQ, HALF), BF16), vm((SEQ, HALF), BF16), *[vm((SEQ, HALF), BF16)] * 3, vm((3, TOK, HALF), BF16),
            vm((2, 2, 4, 4, 4, ROWS, 128), F32), vm((2, 2, ROWS, 128), F32),
        ]
        for part in range(3):
            for phase in range(3):
                scratch += hop_shapes(part, phase)
        scratch += [pltpu.SemaphoreType.DMA((NUM_SEMS,)), pltpu.SemaphoreType.DMA((NUM_SEMS,)),
                    pltpu.SemaphoreType.DMA((NUM_LOCAL,))]
        held = pl.pallas_call(
            lambda *refs: kernel(scale, *refs),
            out_shape=(vm((TOK, DIM), BF16), vm((TOK, DIM), BF16), vm((ROWS, DIM), F32)),
            in_specs=[any_] * 6,
            out_specs=(pl.BlockSpec(memory_space=pltpu.VMEM),) * 3,
            scratch_shapes=scratch,
            name="layer",
            compiler_params=pltpu.CompilerParams(collective_id=0, has_side_effects=True, vmem_limit_bytes=62560000),
        )(x[0], dy[0], wq, wk, wv, wo.reshape(DIM, DIM))
        y, dx, dw = pl.pallas_call(
            write_out,
            out_shape=(jax.ShapeDtypeStruct((TOK, DIM), BF16), jax.ShapeDtypeStruct((TOK, DIM), BF16),
                       jax.ShapeDtypeStruct((ROWS, DIM), F32)),
            in_specs=[pl.BlockSpec(memory_space=pltpu.VMEM)] * 3,
            out_specs=(any_,) * 3,
            scratch_shapes=[pltpu.SemaphoreType.DMA((9,))],
            name="write_out",
            compiler_params=pltpu.CompilerParams(vmem_limit_bytes=16 * 1024 * 1024),
        )(*held)
        return y[None], dx[None], dw

    return jax.shard_map(local, mesh=mesh,
                         in_specs=(act, P(None, None), P(None, None), P(None, None), P(None, None, None), act),
                         out_specs=(act, act, P(("pod", "data"), None)), check_vma=False)
```

```python
import jax
import jax.numpy as jnp
from jax import lax
from jax.experimental import pallas as pl
from jax.experimental.pallas import tpu as pltpu
from jax.sharding import PartitionSpec as P

MESH = pl.DeviceIdType.MESH
F32 = jnp.float32
BF16 = jnp.bfloat16

TOK = 1024
SEQ = 2 * TOK
DIM = 1024
HALF = DIM // 2
GRP = 256
CHUNK = 256
NCH = SEQ // CHUNK
BLK = 512
ROWS = 64

ORDER = (("z", "y", "x"), ("y", "x", "z"), ("x", "z", "y"))
PART_ROWS = ((0, 16), (16, 24), (40, 24))
AXES = ("z", "y", "x")


def dot(a, b):
    return lax.dot_general(a, b, (((1,), (0,)), ((), ())), preferred_element_type=F32)


def dot_t(a, b):
    return lax.dot_general(a, b, (((1,), (1,)), ((), ())), preferred_element_type=F32)


def t_dot(a, b):
    return lax.dot_general(a, b, (((0,), (0,)), ((), ())), preferred_element_type=F32)


NUM_SEMS = 240
NUM_LOCAL = 14
KINDS = {"1A": (0, 2, 0, 1), "1B": (1, 2, 0, -1), "RB": (1, 1, 1, 1), "LA": (0, 3, 2, -1),
         "RA": (0, 1, 1, 1), "LB": (1, 3, 2, -1),
         "O": (slice(None), 2, 0, 2), "R": (slice(None), 1, 1, 1), "L": (slice(None), 3, 2, -1)}
RAW = ("1A", "1B", "RB", "LA")
RING = ("RB", "LA", "RA", "LB")
LAST = ("O", "R", "L")
GENS = {"E0": (0, 0, 3, None), "L0": (None, 3, 1, 0), "E1": (1, 0, 3, None), "L1": (None, 3, 1, 1)}


def when(cond, fn):
    if cond is None:
        fn()
    else:
        pl.when(cond)(fn)


def both(a, b):
    return b if a is None else a if b is None else jnp.logical_and(a, b)


def kernel(scale, x_hbm, dy_hbm, wq_hbm, wk_hbm, wv_hbm, wo_hbm,
           y_ref, dx_ref, dw_ref,
           xf, xt, dyf, wq, wk, wv, wo, sga, sgb, qg, kg, vg,
           kv_raw, qd_raw, oo, o_in, gq, gk, gv, g_in, acc, fin,
           r00, l00, m00, r01, l01, m01, r02, l02, m02,
           r10, l10, m10, r11, l11, m11, r12, l12, m12,
           r20, l20, m20, r21, l21, m21, r22, l22, m22,
           send_sem, recv_sem, local_sem):
    core = lax.axis_index("seq")
    data = lax.axis_index("data")
    me = {"z": lax.div(data, 16), "y": lax.rem(lax.div(data, 4), 4), "x": lax.rem(data, 4)}
    at = {a: [me[a]] + [lax.rem(me[a] + k, 4) for k in (1, 2, 3)] for a in AXES}
    yat = [lax.rem(v, 2) * 2 + lax.div(v, 2) for v in at["y"]]
    stride = {"z": 16, "y": 4, "x": 1}
    away = {a: [data + (at[a][k] - me[a]) * stride[a] for k in range(4)] for a in AXES}
    is_last = [v == 3 for v in at["z"]]
    not_last = [v != 3 for v in at["z"]]
    parity = [[lax.rem(v, 2) == par for v in at["y"]] for par in (0, 1)]
    conds = {}
    other = 1 - core
    hop_bufs = {(0, 0): (r00, l00, m00), (0, 1): (r01, l01, m01), (0, 2): (r02, l02, m02),
                (1, 0): (r10, l10, m10), (1, 1): (r11, l11, m11), (1, 2): (r12, l12, m12),
                (2, 0): (r20, l20, m20), (2, 1): (r21, l21, m21), (2, 2): (r22, l22, m22)}
    sem_ids = {}
    sent = []

    def device(axis, delta):
        return {"data": away[axis][delta % 4], "seq": core}

    partner = {"data": data, "seq": other}

    def remote(name, src, dst, dev):
        k = sem_ids.setdefault(name, len(sem_ids))
        assert k < NUM_SEMS
        return pltpu.make_async_remote_copy(src_ref=src, dst_ref=dst, send_sem=send_sem.at[k],
                                            recv_sem=recv_sem.at[k], device_id=dev, device_id_type=MESH)

    def start(copy):
        copy.start()
        sent.append((copy, None))

    def gen_test(gen, axis, k):
        _, m_lo, _, par = GENS[gen]
        if axis == "z":
            return ("z", m_lo != 0, k)
        if axis == "y" and par is not None:
            return ("y", par, k)
        return None

    def active(gen, part, phase, step):
        tests = [gen_test(gen, axis, 0 if p < phase else step) for p, axis in enumerate(ORDER[part][:phase + 1])]
        key = tuple(sorted(t for t in tests if t is not None))
        if key not in conds:
            cond = None
            for axis, kind, k in key:
                cond = both(cond, (is_last if kind else not_last)[k] if axis == "z" else parity[kind][k])
            conds[key] = cond
        return conds[key]

    def place(part, phase, step):
        where = {}
        for p, a in enumerate(ORDER[part][:phase + 1]):
            k = 0 if p < phase else step
            where[a] = yat[k] if a == "y" else at[a][k]
        return where

    def free_range(gen, axis, msub=None):
        _, m_lo, mn, par = GENS[gen]
        if axis == "z":
            return (m_lo, mn) if msub is None else (msub, 1)
        if axis == "y" and par is not None:
            return 2 * par, 2
        return 0, 4

    def copy_of(gen, part, phase, kind, msub=None):
        h, step, b, direction = KINDS[kind]
        g = GENS[gen][0]
        gsl = pl.ds(0, 2) if g is None else pl.ds(g, 1)
        row0, nr = PART_ROWS[part]
        where, land = place(part, phase, step), [gsl, h]
        for a in AXES:
            if a not in where:
                where[a] = pl.ds(*free_range(gen, a, msub))
                land.append(where[a])
        src = acc.at[(gsl, h, where["z"], where["y"], where["x"], pl.ds(row0, nr), slice(None))]
        return remote((gen, part, phase, kind), src, hop_bufs[part, phase][b].at[tuple(land)],
                      device(ORDER[part][phase], direction))

    def send(gen, part, phase, kind):
        cond = active(gen, part, phase, KINDS[kind][1])
        copy = copy_of(gen, part, phase, kind)
        when(cond, copy.start)
        sent.append((copy, cond))

    def ring_start(gen, kinds, m=None):
        last = m is None or m == 2
        for kind in kinds:
            for part in (1, 2, 0):
                step = KINDS[kind][1]
                cond = active(gen, part, 0, step)
                if ORDER[part][0] == "z":
                    copy = copy_of(gen, part, 0, kind)
                    when(at["z"][step] == (3 if m is None else m), copy.start)
                else:
                    copy = copy_of(gen, part, 0, kind, m)
                    when(cond, copy.start)
                if last:
                    sent.append((copy_of(gen, part, 0, kind), cond))

    def add_into(gen, part, phase, hs, step, bufs):
        row0, nr = PART_ROWS[part]
        g = GENS[gen][0]
        where, land = place(part, phase, step), []
        for a in AXES:
            if a not in where:
                where[a] = pl.ds(*free_range(gen, a))
                land.append(where[a])
        for gi in ((0, 1) if g is None else (g,)):
            for h in hs:
                spot = (gi, h, where["z"], where["y"], where["x"], pl.ds(row0, nr), slice(None))
                total = acc[spot]
                for b in bufs:
                    total = total + b[(gi, h, *land, slice(None), slice(None))]
                acc[spot] = total

    def relay(gens, phase, parts=(1, 2, 0)):
        for part in parts:
            for gen in gens:
                for got, out in (("1A", "RA"), ("1B", "LB")):
                    step = KINDS[out][1]
                    cond = active(gen, part, phase, step)
                    arrived = copy_of(gen, part, phase, got)
                    copy = copy_of(gen, part, phase, out)

                    def go():
                        arrived.wait_recv()
                        add_into(gen, part, phase, (KINDS[out][0],), step, [hop_bufs[part, phase][0]])
                        copy.start()

                    when(cond, go)
                    sent.append((copy, cond))

    def finish(gens, phase, parts=(1, 2, 0)):
        for part in parts:
            for gen in gens:
                arrivals = [copy_of(gen, part, phase, k) for k in (LAST if phase == 2 else RING)]

                def go():
                    for a in arrivals:
                        a.wait_recv()
                    add_into(gen, part, phase, (0, 1), 0, list(hop_bufs[part, phase][0 if phase == 2 else 1:]))

                when(active(gen, part, phase, 0), go)
                if phase < 2:
                    for kind in (RAW if phase == 0 else LAST):
                        send(gen, part, phase + 1, kind)

    def wait_sends(copies):
        for copy, cond in copies:
            when(cond, copy.wait_send)
        copies.clear()

    own0 = pl.multiple_of(core * TOK, TOK)
    oth0 = pl.multiple_of(other * TOK, TOK)
    barrier = pltpu.get_barrier_semaphore()
    for dev in [partner] + [device(a, s) for a in AXES for s in (1, -1)]:
        pl.semaphore_signal(barrier, inc=1, device_id=dev, device_id_type=MESH)
    own_c = pl.ds(pl.multiple_of(core * HALF, HALF), HALF)
    oth_c = pl.ds(pl.multiple_of(other * HALF, HALF), HALF)
    loads = {}

    def load(name, src, dst):
        loads[name] = pltpu.make_async_copy(src, dst, local_sem.at[len(loads)])
        loads[name].start()

    load("x0", x_hbm.at[pl.ds(0, BLK)], xf.at[pl.ds(own0, BLK)])
    for name, src, dst in (("wq", wq_hbm, wq), ("wk", wk_hbm, wk), ("wv", wv_hbm, wv)):
        load(name, src.at[:, own_c], dst)
    load("x1", x_hbm.at[pl.ds(BLK, BLK)], xf.at[pl.ds(own0 + BLK, BLK)])
    load("dy", dy_hbm, dyf.at[pl.ds(own0, TOK)])
    load("wo", wo_hbm.at[own_c], wo)

    lanes = lax.broadcasted_iota(jnp.int32, (1, 128), 1)
    first = (lanes < 64).astype(F32).astype(BF16)
    second = (lanes >= 64).astype(F32).astype(BF16)
    tri = (lax.broadcasted_iota(jnp.int32, (128, 256), 0)
           >= lax.rem(lax.broadcasted_iota(jnp.int32, (128, 256), 1), 128))

    def stacked(a, n):
        part = a[n * 128:n * 128 + 128]
        return jnp.concatenate([part * first, part * second], axis=0)

    def masked(sc):
        top = jnp.where(tri, sc[:128], 0.0).astype(BF16)
        return top if sc.shape[0] == 128 else jnp.concatenate([top, sc[128:].astype(BF16)], axis=0)

    def lower(full, extra):
        return jnp.concatenate([full[:128], full[128:] + extra], axis=0)

    def turned(s0, s1, r):
        wide = t_dot(s0, r)
        tail = jnp.concatenate([s1[:, :128].T, s1[:, 128:].T], axis=1)
        return jnp.concatenate([jnp.where(lanes < 64, wide[:128], wide[128:]), dot(tail, stacked(r, 1))], axis=0)

    block_diag = ((lax.broadcasted_iota(jnp.int32, (128, 128), 0) < 64)
                  == (lax.broadcasted_iota(jnp.int32, (128, 128), 1) < 64))

    def chunk_products(a, b, raw, base, blk):
        for n in range(blk // CHUNK):
            rs = slice(n * CHUNK, (n + 1) * CHUNK)
            p = t_dot(a[rs, :], b[rs, :])
            for j in range(2):
                cs = slice(j * 128, j * 128 + 128)
                raw[lax.div(base, CHUNK) + n, j] = p[cs, cs]

    def project_x(g, base, blk, ready=lambda name: None):
        rows = pl.ds(base, blk)
        gcols = pl.ds(g * GRP, GRP)
        xa = xf[rows, :]
        pre_act = []
        for name, w in (("wq", wq), ("wk", wk)):
            ready(name)
            pre_act.append(dot(xa, w[:, gcols]))
        ready("wv")
        v = dot(xa, wv[:, gcols]).astype(BF16)
        vg[rows, :] = v
        for a, sg, out in ((pre_act[0], sga, qg), (pre_act[1], sgb, kg)):
            s = pl.reciprocal(1.0 + jnp.exp2(a * -1.4426950408889634))
            f = a * s
            kept = f.astype(BF16)
            out[rows, :] = kept
            sg[rows, :] = s + f * (1.0 - s)
        if g == 0:
            xt[:, rows] = xa.T
        chunk_products(kept, v, kv_raw, base, blk)

    def project_dy(g, half, base):
        rows = pl.ds(base, TOK)
        do = dot_t(dyf[rows, :], wo[pl.ds(g * GRP, GRP), :]).astype(BF16)
        dx_ref[:, pl.ds(pl.multiple_of(half * GRP, GRP), GRP)] = do
        chunk_products(qg[rows, :], do, qd_raw, base, TOK)

    def scan_states():
        for raw, side, order in ((kv_raw, 0, range(NCH)), (qd_raw, 1, range(NCH - 1, -1, -1))):
            for j in range(2):
                st = jnp.zeros((128, 128), F32)
                for i in order:
                    y_ref[i * 128:i * 128 + 128, (side * 2 + j) * 128:(side * 2 + j) * 128 + 128] = st.astype(BF16)
                    st = st + jnp.where(block_diag, raw[i, j], 0.0)

    def attend(g, lo, hi):
        def body(i, _):
            rows = pl.ds(pl.multiple_of(i * CHUNK, CHUNK), CHUNK)
            srows = pl.ds(pl.multiple_of(i * 128, 128), 128)
            drows = pl.ds(pl.multiple_of(lax.rem(i, 4) * CHUNK, CHUNK), CHUNK)
            for j in range(2):
                cols = pl.ds(j * 128, 128)
                pre, suf = y_ref[srows, cols], y_ref[srows, pl.ds(256 + j * 128, 128)]
                ocols = pl.ds(g * GRP + j * 128, 128)
                q, k, v = qg[rows, cols], kg[rows, cols], vg[rows, cols]
                do = dx_ref[drows, pl.ds(pl.multiple_of(lax.div(i, 4) * GRP + j * 128, 128), 128)]
                k0, k1, v0, v1 = stacked(k, 0), stacked(k, 1), stacked(v, 0), stacked(v, 1)
                p0, p1 = masked(dot_t(q, k0)), masked(dot_t(q[128:], k1))
                d0, d1 = masked(dot_t(do, v0)), masked(dot_t(do[128:], v1))
                o = lower(dot(p0, v0) + dot(q, pre), dot(p1, v1))
                oo[rows, ocols] = (scale * o).astype(BF16)
                dq = lower(dot(d0, k0) + dot_t(do, pre), dot(d1, k1))
                gq[rows, ocols] = (scale * dq * sga[rows, cols]).astype(BF16)
                dk = dot_t(v, suf) + turned(d0, d1, q)
                gk[rows, ocols] = (scale * dk * sgb[rows, cols]).astype(BF16)
                dv = dot(k, suf) + turned(p0, p1, do)
                gv[rows, ocols] = (scale * dv).astype(BF16)
            return 0

        lax.fori_loop(lo, hi, body, 0, unroll=2)

    def weight_grad(g, m):
        gr = (gq, gk, gv)[m]

        for n in range(2):
            t = dot(xt[n * 512:n * 512 + 512, :], gr[:, pl.ds(g * GRP, GRP)])
            for h in range(2):
                for yy in range(2):
                    for xx in range(4):
                        r = yy * 256 + xx * 64
                        acc[g, h, m, yy * 2 + n, xx] = t[r:r + 64, h * 128:h * 128 + 128]

    def out_weight_grad(g):
        rhs_cols = pl.ds(pl.multiple_of(core * HALF, HALF), HALF)
        for src, who in ((oo, core), (o_in, other)):
            t = t_dot(src[:, pl.ds(g * GRP, GRP)], dyf[:, rhs_cols])
            for gg in range(2):
                for h in range(2):
                    for xx in range(4):
                        c0 = gg * 256 + h * 128
                        acc[gg, h, 3, g * 2 + who, xx] = t[xx * 64:xx * 64 + 64, c0:c0 + 128]

    def share(g):
        cols = pl.ds(g * GRP, GRP)
        o_copy = remote(("o", g), oo.at[:, cols], o_in.at[:, cols], partner)
        start(o_copy)
        g_copies = []
        for m, gr in enumerate((gq, gk, gv)):
            g_copies.append(remote(("g", g, m), gr.at[pl.ds(oth0, TOK), cols], g_in.at[m, :, cols], partner))
            start(g_copies[-1])
        return o_copy, g_copies

    a0 = core * TOK
    with jax.named_scope("barrier"):
        pl.semaphore_wait(barrier, 7)
    x_send = remote("x", x_hbm, xf.at[pl.ds(own0, TOK)], partner)
    dy_send = remote("dy", dy_hbm, dyf.at[pl.ds(own0, TOK)], partner)
    start(x_send)
    start(dy_send)
    with jax.named_scope("load0"):
        loads["x0"].wait()
    project_x(0, pl.multiple_of(a0, BLK), BLK, lambda name: loads[name].wait())
    with jax.named_scope("projA0"):
        loads["x1"].wait()
        project_x(0, pl.multiple_of(a0 + BLK, BLK), BLK)
        for name in ("dy", "wo"):
            loads[name].wait()
        project_dy(0, core, own0)
    with jax.named_scope("xrecv"):
        x_send.wait_recv()
    with jax.named_scope("projB0"):
        for n in range(2):
            project_x(0, pl.multiple_of(oth0 + n * BLK, BLK), BLK)
    with jax.named_scope("dyrecv"):
        dy_send.wait_recv()
    with jax.named_scope("projBd0"):
        project_dy(0, other, oth0)
    with jax.named_scope("scan0"):
        scan_states()
    with jax.named_scope("attend0"):
        attend(0, 0, NCH)
    o_copy0, g_copies0 = share(0)
    with jax.named_scope("wgrad0"):
        for m in range(3):
            weight_grad(0, m)
            ring_start("E0", ("1A", "1B"), m)
    with jax.named_scope("dwo0"):
        o_copy0.wait_recv()
        out_weight_grad(0)
        ring_start("L0", ("1A", "1B"))
        for m in range(3):
            ring_start("E0", ("RB", "LA"), m)
        ring_start("L0", ("RB", "LA"))

    with jax.named_scope("projA1"):
        for n in range(2):
            project_x(1, pl.multiple_of(own0 + n * BLK, BLK), BLK)
        project_dy(1, core, own0)
    with jax.named_scope("r1E0"):
        relay(("E0",), 0)
    with jax.named_scope("projB1"):
        for n in range(2):
            project_x(1, pl.multiple_of(oth0 + n * BLK, BLK), BLK)
        project_dy(1, other, oth0)
    with jax.named_scope("r1L0"):
        relay(("L0",), 0)
    load("wq2", wq_hbm.at[:, oth_c], xf.at[pl.ds(0, DIM), pl.ds(0, HALF)])
    load("wk2", wk_hbm.at[:, oth_c], xf.at[pl.ds(0, DIM), pl.ds(HALF, HALF)])
    load("wv2", wv_hbm.at[:, oth_c], xf.at[pl.ds(DIM, DIM), pl.ds(0, HALF)])
    for n in range(2):
        load(f"wo2{n}", wo_hbm.at[oth_c, pl.ds(n * HALF, HALF)], xf.at[pl.ds(DIM + n * HALF, HALF), pl.ds(HALF, HALF)])
    with jax.named_scope("scan1"):
        scan_states()
    with jax.named_scope("attend1a"):
        attend(1, 0, 4)
    with jax.named_scope("f1_0"):
        finish(("E0", "L0"), 0)
    with jax.named_scope("attend1b"):
        attend(1, 4, 8)
    o_copy1, g_copies1 = share(1)
    with jax.named_scope("r2_0"):
        relay(("E0", "L0"), 1)
    with jax.named_scope("wgrad1"):
        for m in range(3):
            weight_grad(1, m)
            ring_start("E1", ("1A", "1B"), m)
            if m:
                ring_start("E1", ("RB", "LA"), m - 1)
    with jax.named_scope("dwo1"):
        o_copy1.wait_recv()
        out_weight_grad(1)
        ring_start("L1", ("1A", "1B"))
        ring_start("E1", ("RB", "LA"), 2)
        ring_start("L1", ("RB", "LA"))
    with jax.named_scope("f2_0"):
        finish(("E0", "L0"), 1)

    def y_part(r, n):
        rows, cols = pl.ds(pl.multiple_of(own0 + r * HALF, HALF), HALF), pl.ds(n * HALF, HALF)
        t = dot(oo[rows, :], wo[:, cols]) + dot(o_in[rows, :], xf[pl.ds(DIM + n * HALF, HALF), pl.ds(HALF, HALF)])
        y_ref[pl.ds(r * HALF, HALF), cols] = t.astype(BF16)

    def dx_part(r, n):
        rows, cols = pl.ds(pl.multiple_of(own0 + r * HALF, HALF), HALF), pl.ds(n * HALF, HALF)
        t = None
        for m, (gr, w, w2) in enumerate(((gq, wq, xf.at[cols, pl.ds(0, HALF)]), (gk, wk, xf.at[cols, pl.ds(HALF, HALF)]),
                                         (gv, wv, xf.at[pl.ds(DIM + n * HALF, HALF), pl.ds(0, HALF)]))):
            u = dot_t(gr[rows, :], w[cols, :]) + dot_t(g_in[m, pl.ds(r * HALF, HALF), :], w2[...])
            t = u if t is None else t + u
        dx_ref[pl.ds(r * HALF, HALF), cols] = t.astype(BF16)

    for name in ("wq2", "wk2", "wv2", "wo20", "wo21"):
        loads[name].wait()
    with jax.named_scope("Y"):
        for r in range(2):
            for n in range(2):
                y_part(r, n)
    for c in g_copies0 + g_copies1:
        c.wait_recv()
    with jax.named_scope("dX0"):
        dx_part(0, 0)
    with jax.named_scope("r1E1"):
        relay(("E1", "L1"), 0)
    with jax.named_scope("dX1"):
        dx_part(0, 1)
    with jax.named_scope("dX2"):
        dx_part(1, 0)
    with jax.named_scope("f3_0"):
        finish(("E0", "L0"), 2)
    last_gens = ("E1", "L1")
    with jax.named_scope("f1_1z"):
        finish(last_gens, 0, (0,))
    with jax.named_scope("dX3"):
        dx_part(1, 1)
    with jax.named_scope("f1_1"):
        finish(last_gens, 0, (1, 2))
    with jax.named_scope("sends"):
        early = sent[:-36]
        del sent[:-36]
        wait_sends(early)
    with jax.named_scope("r2_1"):
        relay(last_gens, 1, (0, 1, 2))
    with jax.named_scope("f2_1"):
        finish(last_gens, 1, (0, 1, 2))
    with jax.named_scope("f3_1"):
        finish(last_gens, 2)

    final = acc.at[:, :, me["z"], yat[0], me["x"]]
    last = remote("final", final, fin, partner)
    start(last)
    with jax.named_scope("sends2"):
        for g in range(2):
            for h in range(2):
                cols = pl.ds(pl.multiple_of(core * HALF + g * 256 + h * 128, 128), 128)
                dw_ref[:, cols] = acc[g, h, me["z"], yat[0], me["x"]]
        wait_sends(sent)
    with jax.named_scope("last"):
        last.wait_recv()
    for g in range(2):
        for h in range(2):
            cols = pl.ds(pl.multiple_of(other * HALF + g * 256 + h * 128, 128), 128)
            dw_ref[:, cols] = fin[g, h]
    wait_sends(sent)


def hop_shapes(part, phase):
    rest = 2 - phase
    return [pltpu.VMEM((2, 2) + (4,) * rest + (PART_ROWS[part][1], 128), F32)] * 3


def write_out(y_in, dx_in, dw_in, y_out, dx_out, dw_out, sems):
    copies = [pltpu.make_async_copy(dw_in, dw_out, sems.at[8])]
    for n in range(4):
        rows = pl.ds(n * (TOK // 4), TOK // 4)
        copies.append(pltpu.make_async_copy(y_in.at[rows], y_out.at[rows], sems.at[n]))
        copies.append(pltpu.make_async_copy(dx_in.at[rows], dx_out.at[rows], sems.at[4 + n]))
    for c in copies:
        c.start()
    for c in copies:
        c.wait()


def solution(mesh):
    act = P(("pod", "data"), "seq", None)
    scale = float((64 * SEQ) ** -0.5)

    def local(x, wq, wk, wv, wo, dy):
        vm = pltpu.VMEM
        any_ = pl.BlockSpec(memory_space=pl.ANY)
        scratch = [
            vm((SEQ, DIM), BF16), vm((DIM, SEQ), BF16), vm((SEQ, DIM), BF16),
            *[vm((DIM, HALF), BF16)] * 3, vm((HALF, DIM), BF16),
            *[vm((SEQ, GRP), F32)] * 2, *[vm((SEQ, GRP), BF16)] * 3,
            *[vm((NCH, 2, 128, 128), F32)] * 2,
            vm((SEQ, HALF), BF16), vm((SEQ, HALF), BF16), *[vm((SEQ, HALF), BF16)] * 3, vm((3, TOK, HALF), BF16),
            vm((2, 2, 4, 4, 4, ROWS, 128), F32), vm((2, 2, ROWS, 128), F32),
        ]
        for part in range(3):
            for phase in range(3):
                scratch += hop_shapes(part, phase)
        scratch += [pltpu.SemaphoreType.DMA((NUM_SEMS,)), pltpu.SemaphoreType.DMA((NUM_SEMS,)),
                    pltpu.SemaphoreType.DMA((NUM_LOCAL,))]
        held = pl.pallas_call(
            lambda *refs: kernel(scale, *refs),
            out_shape=(vm((TOK, DIM), BF16), vm((TOK, DIM), BF16), vm((ROWS, DIM), F32)),
            in_specs=[any_] * 6,
            out_specs=(pl.BlockSpec(memory_space=pltpu.VMEM),) * 3,
            scratch_shapes=scratch,
            name="layer",
            compiler_params=pltpu.CompilerParams(collective_id=0, has_side_effects=True, vmem_limit_bytes=62560000),
        )(x[0], dy[0], wq, wk, wv, wo.reshape(DIM, DIM))
        y, dx, dw = pl.pallas_call(
            write_out,
            out_shape=(jax.ShapeDtypeStruct((TOK, DIM), BF16), jax.ShapeDtypeStruct((TOK, DIM), BF16),
                       jax.ShapeDtypeStruct((ROWS, DIM), F32)),
            in_specs=[pl.BlockSpec(memory_space=pltpu.VMEM)] * 3,
            out_specs=(any_,) * 3,
            scratch_shapes=[pltpu.SemaphoreType.DMA((9,))],
            name="write_out",
            compiler_params=pltpu.CompilerParams(vmem_limit_bytes=16 * 1024 * 1024),
        )(*held)
        return y[None], dx[None], dw

    return jax.shard_map(local, mesh=mesh,
                         in_specs=(act, P(None, None), P(None, None), P(None, None), P(None, None, None), act),
                         out_specs=(act, act, P(("pod", "data"), None)), check_vma=False)
```
